256 devices in a mesh: row: 8 (over y, core), col: 32 (over z, x).
Axes of the slice: x: 4, y: 4, z: 8, core: 2. Of those that a mesh axis runs over, the one named last changes fastest.
Arguments:
- constraint: bfloat16 [16384, 65536], P('row', 'col'), may hold values from -0.0234375 to 0.0234375
- pattern: int32 [128, 512], P('row', 'col'), may hold values 0 or 1
- objective: float32 [65536, 256], P('col'), may hold values from -31 to 31
- row_bound: float32 [16384, 256], P('row'), may hold values from -31 to 31
- lower_bound: float32 [65536], P('col'), may hold values from -2 to -0.5
- upper_bound: float32 [65536], P('col'), may hold values from 0.5 to 2
Outputs:
- primal: float32 [65536, 256], P('col')
- dual_values: float32 [16384, 256], P('row')
- residual_norms: float32 [256], replicated
The draws below stay inside these ranges and needn't reach their ends.
All inputs are finite; a program needn't handle non-finite values. No bound on the sum of `pattern` on one device may be relied on, other than what follows from the above.
Results may differ from the reference program's by a relative error of at most 0.0019.
Values may be sent and summed in bfloat16 or wider, within the bound.
A program may use at most 128 MiB of HBM per device.

```python
import jax
import jax.numpy as jnp
from jax import lax

BLOCK = 128
K = 256
ITERS = 3
MB = 128
NB = 512
M = 16384
N = 65536


def ramped(key, length, columns):
    first, second = jax.random.split(key)
    ramp_scale = 1.0 + 2.0 * jnp.arange(length, dtype=jnp.float32) / (length - 1)
    rough_scale = jnp.exp(jax.random.uniform(second, (length, 1), jnp.float32, -0.7, 0.7))
    base_values = jnp.clip(jax.random.normal(first, (length, columns), jnp.float32), -5.0, 5.0)
    return base_values * ramp_scale[:, None] * rough_scale


def draw_objective(key, part):
    return ramped(jax.random.fold_in(key, 11), N, K)


def draw_row_bound(key, part):
    return ramped(jax.random.fold_in(key, 23), M, K)


def with_ends(drawn, rng, low, top_value):
    place = [jax.random.randint(jax.random.fold_in(rng, axis), (), 0, length) for axis, length in enumerate(drawn.shape)]
    longest = drawn.shape.index(max(drawn.shape))
    next_to = place[:longest] + [(place[longest] + 1) % drawn.shape[longest]] + place[longest + 1:]
    return drawn.at[tuple(place)].set(low).at[tuple(next_to)].set(top_value)


def level_of(own_key, shape, cuts, low, top_value):
    loudness, own = 1.0, jax.random.fold_in(own_key, 6)
    for dim, shards_of in cuts:
        draws = jnp.exp(jax.random.uniform(jax.random.fold_in(own, dim), (shards_of,), jnp.float32, low / len(cuts), top_value / len(cuts)))
        loudness = loudness * jnp.repeat(draws, shape[dim] // shards_of).reshape([-1 if axis == dim else 1 for axis in range(len(shape))])
    return loudness


def noise(stream_key, extent, scale, bound, cuts=(), kind=jnp.bfloat16):
    drawn = scale * jax.random.normal(stream_key, extent, jnp.float32)
    if cuts:
        drawn = drawn * level_of(stream_key, extent, cuts, -0.22, 0.18)
    return jnp.clip(drawn, -bound, bound).astype(kind)


def setup_inputs(seed: int = 0) -> dict:
    arg_keys = jax.random.split(jax.random.key(seed), 7)
    constraint = noise(arg_keys[0], (M, N), N ** -0.5, 0.0234375, ((0, 8), (1, 32)))
    pattern = with_ends((jax.random.randint(arg_keys[1], (MB, NB), 0, 4) < 3).astype(jnp.int32), jax.random.fold_in(arg_keys[1], 1), 0, 1)
    objective = draw_objective(jax.random.fold_in(arg_keys[6], 71), 0)
    row_bound = draw_row_bound(jax.random.fold_in(arg_keys[6], 71), 0)
    lower_bound = jnp.clip(-2.0 + 1.5 * jax.random.uniform(arg_keys[4], (N,), jnp.float32) ** level_of(arg_keys[4], (N,), ((0, 32),), -0.2, 0.2), -2.0, -0.5)
    upper_bound = jnp.clip(0.5 + 1.5 * jax.random.uniform(arg_keys[5], (N,), jnp.float32) ** level_of(arg_keys[5], (N,), ((0, 32),), -0.2, 0.2), 0.5, 2.0)
    return {"constraint": constraint, "pattern": pattern, "objective": objective, "row_bound": row_bound, "lower_bound": lower_bound, "upper_bound": upper_bound}


step_primal = 0.6
step_dual = 0.6
epsilon = 1e-06

def reference(constraint, pattern, objective, row_bound, lower_bound, upper_bound):
    row_blocks, col_blocks = pattern.shape
    matrix = (constraint.reshape(row_blocks, BLOCK, col_blocks, BLOCK) * pattern.astype(jnp.bfloat16)[:, None, :, None]).reshape(row_blocks * BLOCK, col_blocks * BLOCK)
    primal = jnp.zeros((col_blocks * BLOCK, K), jnp.float32)
    dual_values = jnp.zeros((row_blocks * BLOCK, K), jnp.float32)
    residual_norms = jnp.zeros((K,), jnp.float32)
    for iteration in range(ITERS):
        if iteration == 0:
            gradient = objective
        else:
            gradient = objective - jnp.dot(matrix.T, dual_values.astype(jnp.bfloat16), preferred_element_type=jnp.float32)
        updated = jnp.clip(primal - step_primal * gradient, lower_bound[:, None], upper_bound[:, None])
        extrapolated = (2.0 * updated - primal).astype(jnp.bfloat16)
        slack_rows = row_bound - jnp.dot(matrix, extrapolated, preferred_element_type=jnp.float32)
        dual_values = jnp.maximum(dual_values + step_dual * slack_rows, 0.0)
        violation = lax.optimization_barrier(jnp.sum(jnp.maximum(slack_rows, 0.0) ** 2, axis=0))
        movement = lax.optimization_barrier(jnp.sum((updated - primal) ** 2, axis=0))
        residual_norms = residual_norms + jnp.sqrt(violation / M + epsilon) + jnp.sqrt(movement / N + epsilon)
        primal = updated
    return (primal, dual_values, residual_norms)
```

```python
import functools

import jax
import jax.numpy as jnp
from jax import lax
from jax.experimental import pallas as pl
from jax.experimental.pallas import tpu as pltpu
from jax.sharding import Mesh
from jax.sharding import PartitionSpec as P

MESH = pl.DeviceIdType.MESH
BF16 = jnp.bfloat16
F32 = jnp.float32
BLOCK = 128
ITERS = 3
NY, NC, NZ, NX = 4, 2, 8, 4
ROW = ("y", "c")
COL = ("z", "x")
K = 256
S = 64
HALF = S // 2
GROUP = NX * S
NJ = 4
step_primal = 0.6
step_dual = 0.6
epsilon = 1e-6


def aligned(index, size):
    return pl.ds(pl.multiple_of(index * size, size), size)


def folded(values):
    return jnp.sum(values.reshape(-1, 8, values.shape[-1]), axis=0)


class Ring:
    def __init__(self, axis, groups, from_prev, from_next, half_prev, half_next, sems):
        self.axis, self.groups = axis, groups
        self.me = lax.axis_index(axis)
        self.next = (self.me + 1) % 4
        self.prev = (self.me + 3) % 4
        self.far = (self.me + 2) % 4
        self.from_prev, self.from_next = from_prev, from_next
        self.half_prev, self.half_next = half_prev, half_next
        self.send_sem, self.half_prev_sem, self.half_next_sem, self.prev_sem, self.next_sem, self.gather_sem, self.gather_send = sems

    def copy(self, src, dst, send, recv, to):
        pltpu.make_async_remote_copy(
            src_ref=src, dst_ref=dst, send_sem=send, recv_sem=recv, device_id={self.axis: to}, device_id_type=MESH
        ).start()

    def begin(self, part, s):
        low, high = pl.ds(0, HALF), pl.ds(HALF, HALF)
        self.copy(part.at[s, self.far, low], self.half_prev.at[s], self.send_sem, self.half_prev_sem.at[s], self.next)
        self.copy(part.at[s, self.far, high], self.half_next.at[s], self.send_sem, self.half_next_sem.at[s], self.prev)
        self.copy(part.at[s, self.next, high], self.from_prev.at[s, high], self.send_sem, self.prev_sem.at[s], self.next)
        self.copy(part.at[s, self.prev, low], self.from_next.at[s, low], self.send_sem, self.next_sem.at[s], self.prev)

    def relay(self, part, s):
        low, high = pl.ds(0, HALF), pl.ds(HALF, HALF)
        arrived(self.half_prev.at[s], self.half_prev_sem.at[s])
        part[s, self.next, low] = (part[s, self.next, low].astype(F32) + self.half_prev[s].astype(F32)).astype(BF16)
        self.copy(part.at[s, self.next, low], self.from_prev.at[s, low], self.send_sem, self.prev_sem.at[s], self.next)
        arrived(self.half_next.at[s], self.half_next_sem.at[s])
        part[s, self.prev, high] = (part[s, self.prev, high].astype(F32) + self.half_next[s].astype(F32)).astype(BF16)
        self.copy(part.at[s, self.prev, high], self.from_next.at[s, high], self.send_sem, self.next_sem.at[s], self.prev)

    def total(self, part, s):
        arrived(self.from_prev.at[s], self.prev_sem.at[s])
        arrived(self.from_next.at[s], self.next_sem.at[s])
        return part[s, self.me].astype(F32) + self.from_prev[s].astype(F32) + self.from_next[s].astype(F32)

    def gather_begin(self, piece, s):
        low, high = pl.ds(0, HALF), pl.ds(HALF, HALF)
        mine = piece(s, self.me)
        self.copy(mine.at[low], mine.at[low], self.gather_send, self.gather_sem.at[0, s], self.next)
        self.copy(mine.at[high], mine.at[high], self.gather_send, self.gather_sem.at[1, s], self.prev)
        self.copy(mine.at[high], mine.at[high], self.gather_send, self.gather_sem.at[2, s], self.next)
        self.copy(mine.at[low], mine.at[low], self.gather_send, self.gather_sem.at[3, s], self.prev)

    def gather_relay(self, piece, s):
        low, high = pl.ds(0, HALF), pl.ds(HALF, HALF)
        left, right = piece(s, self.prev), piece(s, self.next)
        arrived(left.at[low], self.gather_sem.at[0, s])
        self.copy(left.at[low], left.at[low], self.gather_send, self.gather_sem.at[4, s], self.next)
        arrived(right.at[high], self.gather_sem.at[1, s])
        self.copy(right.at[high], right.at[high], self.gather_send, self.gather_sem.at[5, s], self.prev)

    def gather_end(self, piece, s):
        low, high = pl.ds(0, HALF), pl.ds(HALF, HALF)
        left, right, far = piece(s, self.prev), piece(s, self.next), piece(s, self.far)
        arrived(left.at[high], self.gather_sem.at[2, s])
        arrived(right.at[low], self.gather_sem.at[3, s])
        arrived(far.at[low], self.gather_sem.at[4, s])
        arrived(far.at[high], self.gather_sem.at[5, s])

    def drain_sum(self, part):
        view = part.at[:, pl.ds(0, 3)]
        arrived(view, self.send_sem)

    def drain_gather(self, part):
        view = part.at[:, pl.ds(0, 3)]
        arrived(view, self.gather_send)


def arrived(ref, sem):
    pltpu.make_async_copy(ref, ref, sem).wait()


SCRATCH = dict(
    matrix=pltpu.VMEM((2048, 2048), BF16),
    turned=pltpu.VMEM((2048, 2048), BF16),
    objective=pltpu.VMEM((2048, K), F32),
    bound=pltpu.VMEM((2048, K), F32),
    primal=pltpu.VMEM((2048, K), F32),
    dual=pltpu.VMEM((2048, K), F32),
    extra=pltpu.VMEM((2048, K), BF16),
    dual_bf=pltpu.VMEM((2048, K), BF16),
    lower=pltpu.VMEM((2048, BLOCK), F32),
    upper=pltpu.VMEM((2048, BLOCK), F32),
    part_x=pltpu.VMEM((NZ, NX, S, K), BF16),
    x_from_prev=pltpu.VMEM((3, NZ, S, K), BF16),
    x_from_next=pltpu.VMEM((3, NZ, S, K), BF16),
    x_half_prev=pltpu.VMEM((3, NZ, HALF, K), BF16),
    x_half_next=pltpu.VMEM((3, NZ, HALF, K), BF16),
    z_send=pltpu.VMEM((NZ, S, K), BF16),
    z_recv=pltpu.VMEM((3, NZ, S, K), BF16),
    share=pltpu.VMEM((S, K), F32),
    rows=pltpu.VMEM((3, NZ, NX, S, K), BF16),
    core_send=pltpu.VMEM((NJ, NY, S, K), BF16),
    core_own=pltpu.VMEM((NJ, NY, S, K), F32),
    core_recv=pltpu.VMEM((2, NJ, NY, S, K), BF16),
    part_y=pltpu.VMEM((NJ, NY, S, K), BF16),
    y_from_prev=pltpu.VMEM((2, NJ, S, K), BF16),
    y_from_next=pltpu.VMEM((2, NJ, S, K), BF16),
    y_half_prev=pltpu.VMEM((2, NJ, HALF, K), BF16),
    y_half_next=pltpu.VMEM((2, NJ, HALF, K), BF16),
    cols=pltpu.VMEM((2, NJ, NC, NY, S, K), BF16),
    violation=pltpu.VMEM((3, 8, K), F32),
    movement=pltpu.VMEM((3, 8, K), F32),
    violation_own=pltpu.VMEM((8, K), F32),
    violation_pair=pltpu.VMEM((8, K), F32),
    violation_core=pltpu.VMEM((8, K), F32),
    violation_y=pltpu.VMEM((4, 8, K), F32),
    movement_own=pltpu.VMEM((8, K), F32),
    movement_row=pltpu.VMEM((8, K), F32),
    movement_x=pltpu.VMEM((4, 8, K), F32),
    movement_z=pltpu.VMEM((8, 8, K), F32),
    load_sem=pltpu.SemaphoreType.DMA((16,)),
    out_sem=pltpu.SemaphoreType.DMA((2,)),
    x_send_sem=pltpu.SemaphoreType.DMA((3,)),
    x_half_prev_sem=pltpu.SemaphoreType.DMA((3, NZ)),
    x_half_next_sem=pltpu.SemaphoreType.DMA((3, NZ)),
    x_prev_sem=pltpu.SemaphoreType.DMA((3, NZ)),
    x_next_sem=pltpu.SemaphoreType.DMA((3, NZ)),
    x_gather_sem=pltpu.SemaphoreType.DMA((3, 6, NZ)),
    x_gather_send=pltpu.SemaphoreType.DMA((3,)),
    z_send_sem=pltpu.SemaphoreType.DMA((3,)),
    z_recv_sem=pltpu.SemaphoreType.DMA((3, NZ)),
    z_gather_send=pltpu.SemaphoreType.DMA((3,)),
    z_gather_sem=pltpu.SemaphoreType.DMA((3, NZ)),
    core_send_sem=pltpu.SemaphoreType.DMA((2,)),
    core_recv_sem=pltpu.SemaphoreType.DMA((2, NJ)),
    core_gather_send=pltpu.SemaphoreType.DMA((2,)),
    core_gather_sem=pltpu.SemaphoreType.DMA((2, NJ)),
    y_send_sem=pltpu.SemaphoreType.DMA((2,)),
    y_half_prev_sem=pltpu.SemaphoreType.DMA((2, NJ)),
    y_half_next_sem=pltpu.SemaphoreType.DMA((2, NJ)),
    y_prev_sem=pltpu.SemaphoreType.DMA((2, NJ)),
    y_next_sem=pltpu.SemaphoreType.DMA((2, NJ)),
    y_gather_sem=pltpu.SemaphoreType.DMA((2, 6, NJ)),
    y_gather_send=pltpu.SemaphoreType.DMA((2,)),
    stat_send_sem=pltpu.SemaphoreType.DMA((4,)),
    stat_x_sem=pltpu.SemaphoreType.DMA((4,)),
    stat_z_sem=pltpu.SemaphoreType.DMA((8,)),
    stat_y_sem=pltpu.SemaphoreType.DMA((4,)),
    stat_c_sem=pltpu.SemaphoreType.DMA((1,)),
)


class Box:
    pass


def kernel(constraint, pattern, objective, row_bound, lower, upper, primal_out, dual_out, norms, *refs):
    b = Box()
    b.__dict__.update(zip(SCRATCH, refs))
    y, c, z, x = (lax.axis_index(name) for name in ("y", "c", "z", "x"))
    other = 1 - c

    barrier = pltpu.get_barrier_semaphore()
    peers = 0
    for name, size, me in (("y", NY, y), ("c", NC, c), ("z", NZ, z), ("x", NX, x)):
        for step in range(1, size):
            pl.semaphore_signal(barrier, inc=1, device_id={name: (me + step) % size}, device_id_type=MESH)
            peers += 1

    def z_target(s):
        return (z + jnp.where(s % 2 == 1, 4 - (s + 1) // 2, 4 + s // 2)) % NZ

    def z_source(s):
        return (z + jnp.where(s % 2 == 1, (s + 1) // 2, NZ - s // 2)) % NZ

    load_objective = pltpu.make_async_copy(objective, b.objective, b.load_sem.at[8])
    load_objective.start()

    def load_matrix(s):
        group = aligned(z_target(s), GROUP)
        return pltpu.make_async_copy(constraint.at[group], b.matrix.at[group], b.load_sem.at[s])

    for s in range(NZ):
        load_matrix(s).start()
    load_bound = pltpu.make_async_copy(row_bound, b.bound, b.load_sem.at[9])
    load_bound.start()

    def spread(i, carry):
        at = aligned(i, BLOCK)
        b.lower[at] = jnp.broadcast_to(lower[pl.ds(i, 1)], (BLOCK, BLOCK)).T
        b.upper[at] = jnp.broadcast_to(upper[pl.ds(i, 1)], (BLOCK, BLOCK)).T
        return carry

    lax.fori_loop(0, 16, spread, 0)

    def wide(values):
        return jnp.concatenate([values, values], axis=1)

    def new_primal(at, gradient, it):
        low, high = wide(b.lower[at]), wide(b.upper[at])
        if it == 0:
            updated = jnp.clip(-step_primal * gradient, low, high)
            moved = updated
            b.extra[at] = (2.0 * updated).astype(BF16)
        else:
            before = b.primal[at]
            updated = jnp.clip(before - step_primal * gradient, low, high)
            moved = updated - before
            b.extra[at] = (2.0 * updated - before).astype(BF16)
        b.primal[at] = updated
        b.movement[it] += folded(moved * moved)

    b.movement[...] = jnp.zeros_like(b.movement)
    b.violation[...] = jnp.zeros_like(b.violation)

    load_objective.wait()

    def first(i, carry):
        at = aligned(i, GROUP)
        new_primal(at, b.objective[at], 0)
        return carry

    lax.fori_loop(0, 8, first, 0)

    def mask_group(group):
        for h in range(2):
            at = aligned(group * 2 + h, BLOCK)
            for j in range(16):
                keep = pattern[group * 2 + h, j].astype(F32).astype(BF16)
                cols = pl.ds(j * BLOCK, BLOCK)
                b.matrix[at, cols] = b.matrix[at, cols] * keep

    def turn_group(group):
        eye = jnp.where(
            lax.broadcasted_iota(jnp.int32, (256, 256), 0) == lax.broadcasted_iota(jnp.int32, (256, 256), 1), 1.0, 0.0
        ).astype(BF16)
        at = aligned(group, GROUP)
        for j in range(8):
            cols = pl.ds(j * 256, 256)
            b.turned[cols, at] = lax.dot_general(
                eye, b.matrix[at, cols], (((1,), (1,)), ((), ())), preferred_element_type=F32
            ).astype(BF16)

    def column_sum(it):
        ring = Ring(
            "x", NZ, b.x_from_prev.at[it], b.x_from_next.at[it], b.x_half_prev.at[it], b.x_half_next.at[it],
            (b.x_send_sem.at[it], b.x_half_prev_sem.at[it], b.x_half_next_sem.at[it], b.x_prev_sem.at[it],
             b.x_next_sem.at[it], b.x_gather_sem.at[it], b.x_gather_send.at[it]),
        )
        rows = b.rows.at[it]

        def piece(group, owner):
            return rows.at[group, owner]

        def z_copy(s):
            return pltpu.make_async_remote_copy(
                src_ref=b.z_send.at[s], dst_ref=b.z_recv.at[it, s], send_sem=b.z_send_sem.at[it],
                recv_sem=b.z_recv_sem.at[it, s], device_id={"z": z_target(s)}, device_id_type=MESH,
            )

        def summing(t, carry):
            @pl.when(t < NZ)
            def _():
                group = z_target(t)
                if it == 0:
                    load_matrix(t).wait()
                    mask_group(group)
                product = jnp.dot(b.matrix[aligned(group, GROUP)], b.extra[...], preferred_element_type=F32)
                b.part_x[t] = product.astype(BF16).reshape(NX, S, K)
                ring.begin(b.part_x, t)
                if it == 0:
                    turn_group(group)

            @pl.when((t >= 2) & (t < NZ + 2))
            def _():
                ring.relay(b.part_x, t - 2)

            @pl.when(t >= 4)
            def _():
                s = t - 4
                total = ring.total(b.part_x, s)

                @pl.when(s < NZ - 1)
                def _():
                    b.z_send[s] = total.astype(BF16)
                    z_copy(s).start()

                @pl.when(s == NZ - 1)
                def _():
                    b.share[...] = total

            return carry

        lax.fori_loop(0, NZ + 4, summing, 0)

        def adding(s, carry):
            arrived(b.z_recv.at[it, s], b.z_recv_sem.at[it, s])
            b.share[...] += b.z_recv[it, s].astype(F32)
            return carry

        lax.fori_loop(0, NZ - 1, adding, 0)
        rows[z, x] = b.share[...].astype(BF16)

        def z_spread(s, carry):
            to = z_source(s)
            mine = piece(z, x)
            pltpu.make_async_remote_copy(
                src_ref=mine, dst_ref=mine, send_sem=b.z_gather_send.at[it], recv_sem=b.z_gather_sem.at[it, z],
                device_id={"z": to}, device_id_type=MESH,
            ).start()
            return carry

        lax.fori_loop(1, NZ, z_spread, 0)

        if it == 0:
            load_bound.wait()

        def gathering(t, carry):
            @pl.when(t < NZ)
            def _():
                group = z_source(t)

                @pl.when(t > 0)
                def _():
                    arrived(piece(group, x), b.z_gather_sem.at[it, group])

                ring.gather_begin(piece, group)

            @pl.when((t >= 2) & (t < NZ + 2))
            def _():
                ring.gather_relay(piece, z_source(t - 2))

            @pl.when(t >= 4)
            def _():
                group = z_source(t - 4)
                ring.gather_end(piece, group)
                at = aligned(group, GROUP)
                slack = b.bound[at] - rows[group].reshape(GROUP, K).astype(F32)
                over = jnp.maximum(slack, 0.0)
                b.violation[it] += folded(over * over)
                if it == 0:
                    dual = jnp.maximum(step_dual * slack, 0.0)
                else:
                    dual = jnp.maximum(b.dual[at] + step_dual * slack, 0.0)
                b.dual[at] = dual
                if it < ITERS - 1:
                    b.dual_bf[at] = dual.astype(BF16)
                else:
                    pltpu.make_async_copy(b.dual.at[at], dual_out.at[at], b.out_sem.at[1]).start()

            return carry

        lax.fori_loop(0, NZ + 4, gathering, 0)
        ring.drain_sum(b.part_x)
        ring.drain_gather(b.part_x)
        arrived(b.z_send.at[pl.ds(0, NZ - 1)], b.z_send_sem.at[it])
        arrived(b.z_send.at[pl.ds(0, NZ - 1)], b.z_gather_send.at[it])

    def row_sum(it):
        n = it - 1
        ring = Ring(
            "y", NJ, b.y_from_prev.at[n], b.y_from_next.at[n], b.y_half_prev.at[n], b.y_half_next.at[n],
            (b.y_send_sem.at[n], b.y_half_prev_sem.at[n], b.y_half_next_sem.at[n], b.y_prev_sem.at[n],
             b.y_next_sem.at[n], b.y_gather_sem.at[n], b.y_gather_send.at[n]),
        )
        cols = b.cols.at[n]

        def piece(j, owner):
            return cols.at[j, c, owner]

        def swap(src, dst, send, recv):
            pltpu.make_async_remote_copy(
                src_ref=src, dst_ref=dst, send_sem=send, recv_sem=recv, device_id={"c": other}, device_id_type=MESH
            ).start()

        def product(j, core):
            return jnp.dot(b.turned[aligned(j * 2 + core, GROUP)], b.dual_bf[...], preferred_element_type=F32)

        def update(j, core):
            at = aligned(j * 2 + core, GROUP)
            new_primal(at, b.objective[at] - cols[j, core].reshape(GROUP, K).astype(F32), it)

        def body(t, carry):
            @pl.when(t < NJ)
            def _():
                b.core_send[t] = product(t, other).astype(BF16).reshape(NY, S, K)
                swap(b.core_send.at[t], b.core_recv.at[n, t], b.core_send_sem.at[n], b.core_recv_sem.at[n, t])
                b.core_own[t] = product(t, c).reshape(NY, S, K)

            @pl.when((t >= 1) & (t < NJ + 1))
            def _():
                j = t - 1
                arrived(b.core_recv.at[n, j], b.core_recv_sem.at[n, j])
                b.part_y[j] = (b.core_own[j] + b.core_recv[n, j].astype(F32)).astype(BF16)
                ring.begin(b.part_y, j)

            @pl.when((t >= 3) & (t < NJ + 3))
            def _():
                ring.relay(b.part_y, t - 3)

            @pl.when((t >= 5) & (t < NJ + 5))
            def _():
                j = t - 5
                cols[j, c, y] = ring.total(b.part_y, j).astype(BF16)
                ring.gather_begin(piece, j)

            @pl.when((t >= 7) & (t < NJ + 7))
            def _():
                ring.gather_relay(piece, t - 7)

            @pl.when((t >= 9) & (t < NJ + 9))
            def _():
                j = t - 9
                ring.gather_end(piece, j)
                swap(cols.at[j, c], cols.at[j, c], b.core_gather_send.at[n], b.core_gather_sem.at[n, j])
                update(j, c)

            @pl.when(t >= 10)
            def _():
                j = t - 10
                arrived(cols.at[j, other], b.core_gather_sem.at[n, j])
                update(j, other)

            return carry

        lax.fori_loop(0, NJ + 10, body, 0)
        ring.drain_sum(b.part_y)
        ring.drain_gather(b.part_y)
        arrived(b.core_send, b.core_send_sem.at[n])
        arrived(b.core_send, b.core_gather_send.at[n])

    def stat_copy(src, dst, send, recv, to):
        pltpu.make_async_remote_copy(
            src_ref=src, dst_ref=dst, send_sem=b.stat_send_sem.at[send], recv_sem=recv, device_id=to, device_id_type=MESH
        ).start()

    def three_rows(parts):
        sums = [jnp.sum(parts[i], axis=0, keepdims=True) for i in range(3)]
        return jnp.concatenate(sums + [jnp.zeros((5, K), F32)], axis=0)

    pl.semaphore_wait(barrier, peers)
    column_sum(0)
    row_sum(1)
    column_sum(1)
    row_sum(2)

    save_primal = pltpu.make_async_copy(b.primal, primal_out, b.out_sem.at[0])
    save_primal.start()
    b.movement_own[...] = three_rows(b.movement)
    for step in range(1, NX):
        stat_copy(b.movement_own, b.movement_x.at[step], 0, b.stat_x_sem.at[step], {"x": (x + step) % NX})

    column_sum(2)

    b.violation_own[...] = three_rows(b.violation)
    stat_copy(b.violation_own, b.violation_core, 2, b.stat_c_sem.at[0], {"c": other})
    row = b.movement_own[...]
    for step in range(1, NX):
        arrived(b.movement_x.at[step], b.stat_x_sem.at[step])
        row += b.movement_x[step]
    b.movement_row[...] = row
    for step in range(1, NZ):
        stat_copy(b.movement_row, b.movement_z.at[step], 1, b.stat_z_sem.at[step], {"z": (z + step) % NZ})
    arrived(b.violation_core, b.stat_c_sem.at[0])
    pair = b.violation_own[...] + b.violation_core[...]
    b.violation_pair[...] = pair
    for step in range(1, NY):
        stat_copy(b.violation_pair, b.violation_y.at[step], 3, b.stat_y_sem.at[step], {"y": (y + step) % NY})

    moved = b.movement_row[...]
    for step in range(1, NZ):
        arrived(b.movement_z.at[step], b.stat_z_sem.at[step])
        moved += b.movement_z[step]
    for step in range(1, NY):
        arrived(b.violation_y.at[step], b.stat_y_sem.at[step])
        pair += b.violation_y[step]
    each = jnp.sqrt(pair / (2048 * NY * NC) + epsilon) + jnp.sqrt(moved / (2048 * NZ * NX) + epsilon)
    norms[...] = each[0:1] + each[1:2] + each[2:3]

    arrived(b.movement_x.at[pl.ds(1, 3)], b.stat_send_sem.at[0])
    arrived(b.movement_z.at[pl.ds(1, 7)], b.stat_send_sem.at[1])
    arrived(b.violation_core, b.stat_send_sem.at[2])
    arrived(b.violation_y.at[pl.ds(1, 3)], b.stat_send_sem.at[3])
    save_primal.wait()
    arrived(b.dual, b.out_sem.at[1])


def on_device(constraint, pattern, objective, row_bound, lower_bound, upper_bound):
    primal, dual, norms = pl.pallas_call(
        kernel,
        out_shape=(
            jax.ShapeDtypeStruct((2048, K), F32),
            jax.ShapeDtypeStruct((2048, K), F32),
            jax.ShapeDtypeStruct((1, K), F32),
        ),
        in_specs=[
            pl.BlockSpec(memory_space=pl.ANY),
            pl.BlockSpec(memory_space=pltpu.SMEM),
            pl.BlockSpec(memory_space=pl.ANY),
            pl.BlockSpec(memory_space=pl.ANY),
            pl.BlockSpec(memory_space=pltpu.VMEM),
            pl.BlockSpec(memory_space=pltpu.VMEM),
        ],
        out_specs=(
            pl.BlockSpec(memory_space=pl.ANY),
            pl.BlockSpec(memory_space=pl.ANY),
            pl.BlockSpec(memory_space=pltpu.VMEM),
        ),
        scratch_shapes=list(SCRATCH.values()),
        compiler_params=pltpu.CompilerParams(
            collective_id=0, has_side_effects=True, vmem_limit_bytes=62 * 1024 * 1024
        ),
        name="pdhg",
    )(constraint, pattern, objective, row_bound, lower_bound.reshape(16, BLOCK), upper_bound.reshape(16, BLOCK))
    return primal, dual, norms.reshape(K)


def solution(mesh):
    torus = Mesh(mesh.devices.reshape(NY, NC, NZ, NX), ("y", "c", "z", "x"))
    in_specs = (P(ROW, COL), P(ROW, COL), P(COL, None), P(ROW, None), P(COL), P(COL))
    out_specs = (P(COL, None), P(ROW, None), P())
    return jax.shard_map(on_device, mesh=torus, in_specs=in_specs, out_specs=out_specs, check_vma=False)
```

```python
import functools

import jax
import jax.numpy as jnp
from jax import lax
from jax.experimental import pallas as pl
from jax.experimental.pallas import tpu as pltpu
from jax.sharding import Mesh
from jax.sharding import PartitionSpec as P

MESH = pl.DeviceIdType.MESH
BF16 = jnp.bfloat16
F32 = jnp.float32
BLOCK = 128
ITERS = 3
NY, NC, NZ, NX = 4, 2, 8, 4
ROW = ("y", "c")
COL = ("z", "x")
K = 256
S = 64
HALF = S // 2
GROUP = NX * S
NJ = 4
LS = 4
LG = 4
LR = 3
FAR_X = 6
FAR_Y = 3
step_primal = 0.6
step_dual = 0.6
epsilon = 1e-6


def aligned(index, size):
    return pl.ds(pl.multiple_of(index * size, size), size)


def folded(values):
    return jnp.sum(values.reshape(-1, 8, values.shape[-1]), axis=0)


class Ring:
    def __init__(self, axis, groups, from_prev, from_next, half_prev, half_next, sems):
        self.axis, self.groups = axis, groups
        self.me = lax.axis_index(axis)
        self.next = (self.me + 1) % 4
        self.prev = (self.me + 3) % 4
        self.far = (self.me + 2) % 4
        self.from_prev, self.from_next = from_prev, from_next
        self.half_prev, self.half_next = half_prev, half_next
        self.send_sem, self.half_prev_sem, self.half_next_sem, self.prev_sem, self.next_sem, self.gather_sem, self.gather_send = sems

    def copy(self, src, dst, send, recv, to):
        pltpu.make_async_remote_copy(
            src_ref=src, dst_ref=dst, send_sem=send, recv_sem=recv, device_id={self.axis: to}, device_id_type=MESH
        ).start()

    def begin(self, part, s):
        low, high = pl.ds(0, HALF), pl.ds(HALF, HALF)
        self.copy(part.at[s, self.far, low], self.half_prev.at[s], self.send_sem, self.half_prev_sem.at[s], self.next)
        self.copy(part.at[s, self.far, high], self.half_next.at[s], self.send_sem, self.half_next_sem.at[s], self.prev)
        self.copy(part.at[s, self.next, high], self.from_prev.at[s, high], self.send_sem, self.prev_sem.at[s], self.next)
        self.copy(part.at[s, self.prev, low], self.from_next.at[s, low], self.send_sem, self.next_sem.at[s], self.prev)

    def relay(self, part, s):
        low, high = pl.ds(0, HALF), pl.ds(HALF, HALF)
        arrived(self.half_prev.at[s], self.half_prev_sem.at[s])
        part[s, self.next, low] = (part[s, self.next, low].astype(F32) + self.half_prev[s].astype(F32)).astype(BF16)
        self.copy(part.at[s, self.next, low], self.from_prev.at[s, low], self.send_sem, self.prev_sem.at[s], self.next)
        arrived(self.half_next.at[s], self.half_next_sem.at[s])
        part[s, self.prev, high] = (part[s, self.prev, high].astype(F32) + self.half_next[s].astype(F32)).astype(BF16)
        self.copy(part.at[s, self.prev, high], self.from_next.at[s, high], self.send_sem, self.next_sem.at[s], self.prev)

    def total(self, part, s):
        arrived(self.from_prev.at[s], self.prev_sem.at[s])
        arrived(self.from_next.at[s], self.next_sem.at[s])
        return part[s, self.me].astype(F32) + self.from_prev[s].astype(F32) + self.from_next[s].astype(F32)

    def gather_begin(self, piece, s, direct):
        low, high = pl.ds(0, HALF), pl.ds(HALF, HALF)
        mine = piece(s, self.me)
        self.copy(mine.at[low], mine.at[low], self.gather_send, self.gather_sem.at[0, s], self.next)
        self.copy(mine.at[high], mine.at[high], self.gather_send, self.gather_sem.at[1, s], self.prev)
        self.copy(mine.at[high], mine.at[high], self.gather_send, self.gather_sem.at[2, s], self.next)
        self.copy(mine.at[low], mine.at[low], self.gather_send, self.gather_sem.at[3, s], self.prev)

        @pl.when(direct)
        def _():
            self.copy(mine.at[low], mine.at[low], self.gather_send, self.gather_sem.at[4, s], self.far)
            self.copy(mine.at[high], mine.at[high], self.gather_send, self.gather_sem.at[5, s], self.far)

    def gather_relay(self, piece, s, direct):
        low, high = pl.ds(0, HALF), pl.ds(HALF, HALF)
        left, right = piece(s, self.prev), piece(s, self.next)
        arrived(left.at[low], self.gather_sem.at[0, s])

        @pl.when(jnp.logical_not(direct))
        def _():
            self.copy(left.at[low], left.at[low], self.gather_send, self.gather_sem.at[4, s], self.next)

        arrived(right.at[high], self.gather_sem.at[1, s])

        @pl.when(jnp.logical_not(direct))
        def _():
            self.copy(right.at[high], right.at[high], self.gather_send, self.gather_sem.at[5, s], self.prev)

    def gather_end(self, piece, s):
        low, high = pl.ds(0, HALF), pl.ds(HALF, HALF)
        left, right, far = piece(s, self.prev), piece(s, self.next), piece(s, self.far)
        arrived(left.at[high], self.gather_sem.at[2, s])
        arrived(right.at[low], self.gather_sem.at[3, s])
        arrived(far.at[low], self.gather_sem.at[4, s])
        arrived(far.at[high], self.gather_sem.at[5, s])

    def drain_sum(self, part):
        view = part.at[:, pl.ds(0, 3)]
        arrived(view, self.send_sem)

    def drain_gather(self, part):
        view = part.at[:, pl.ds(0, 3)]
        arrived(view, self.gather_send)


def arrived(ref, sem):
    pltpu.make_async_copy(ref, ref, sem).wait()


SCRATCH = dict(
    matrix=pltpu.VMEM((2048, 2048), BF16),
    turned=pltpu.VMEM((2048, 2048), BF16),
    objective=pltpu.VMEM((2048, K), F32),
    bound=pltpu.VMEM((2048, K), F32),
    extra=pltpu.VMEM((2048, K), BF16),
    dual_bf=pltpu.VMEM((2048, K), BF16),
    lower=pltpu.VMEM((2048, BLOCK), F32),
    upper=pltpu.VMEM((2048, BLOCK), F32),
    part_x=pltpu.VMEM((NZ, NX, S, K), BF16),
    x_from_prev=pltpu.VMEM((3, NZ, S, K), BF16),
    x_from_next=pltpu.VMEM((3, NZ, S, K), BF16),
    x_half_prev=pltpu.VMEM((3, NZ, HALF, K), BF16),
    x_half_next=pltpu.VMEM((3, NZ, HALF, K), BF16),
    z_send=pltpu.VMEM((NZ, S, K), BF16),
    z_recv=pltpu.VMEM((3, NZ, S, K), BF16),
    share=pltpu.VMEM((S, K), F32),
    rows=pltpu.VMEM((3, NZ, NX, S, K), BF16),
    core_send=pltpu.VMEM((NJ, NY, S, K), BF16),
    core_recv=pltpu.VMEM((2, NJ, NY, S, K), BF16),
    part_y=pltpu.VMEM((NJ, NY, S, K), BF16),
    y_from_prev=pltpu.VMEM((2, NJ, S, K), BF16),
    y_from_next=pltpu.VMEM((2, NJ, S, K), BF16),
    y_half_prev=pltpu.VMEM((2, NJ, HALF, K), BF16),
    y_half_next=pltpu.VMEM((2, NJ, HALF, K), BF16),
    cols=pltpu.VMEM((2, NJ, NC, NY, S, K), BF16),
    violation=pltpu.VMEM((3, 8, K), F32),
    movement=pltpu.VMEM((3, 8, K), F32),
    stat_own=pltpu.VMEM((8, K), F32),
    stat_pair=pltpu.VMEM((8, K), F32),
    stat_row=pltpu.VMEM((8, K), F32),
    stat_col=pltpu.VMEM((8, K), F32),
    stat_core=pltpu.VMEM((8, K), F32),
    stat_y=pltpu.VMEM((4, 8, K), F32),
    stat_z=pltpu.VMEM((8, 8, K), F32),
    stat_x=pltpu.VMEM((4, 8, K), F32),
    kept=pltpu.VMEM((8, K), F32),
    load_sem=pltpu.SemaphoreType.DMA((16,)),
    x_send_sem=pltpu.SemaphoreType.DMA((3,)),
    x_half_prev_sem=pltpu.SemaphoreType.DMA((3, NZ)),
    x_half_next_sem=pltpu.SemaphoreType.DMA((3, NZ)),
    x_prev_sem=pltpu.SemaphoreType.DMA((3, NZ)),
    x_next_sem=pltpu.SemaphoreType.DMA((3, NZ)),
    x_gather_sem=pltpu.SemaphoreType.DMA((3, 6, NZ)),
    x_gather_send=pltpu.SemaphoreType.DMA((3,)),
    z_send_sem=pltpu.SemaphoreType.DMA((3,)),
    z_recv_sem=pltpu.SemaphoreType.DMA((3, NZ)),
    z_gather_send=pltpu.SemaphoreType.DMA((3,)),
    z_gather_sem=pltpu.SemaphoreType.DMA((3, NZ)),
    core_send_sem=pltpu.SemaphoreType.DMA((2,)),
    core_recv_sem=pltpu.SemaphoreType.DMA((2, NJ)),
    core_gather_send=pltpu.SemaphoreType.DMA((2,)),
    core_gather_sem=pltpu.SemaphoreType.DMA((2, NJ)),
    y_send_sem=pltpu.SemaphoreType.DMA((2,)),
    y_half_prev_sem=pltpu.SemaphoreType.DMA((2, NJ)),
    y_half_next_sem=pltpu.SemaphoreType.DMA((2, NJ)),
    y_prev_sem=pltpu.SemaphoreType.DMA((2, NJ)),
    y_next_sem=pltpu.SemaphoreType.DMA((2, NJ)),
    y_gather_sem=pltpu.SemaphoreType.DMA((2, 6, NJ)),
    y_gather_send=pltpu.SemaphoreType.DMA((2,)),
    stat_send_sem=pltpu.SemaphoreType.DMA((4,)),
    stat_x_sem=pltpu.SemaphoreType.DMA((4,)),
    stat_z_sem=pltpu.SemaphoreType.DMA((8,)),
    stat_y_sem=pltpu.SemaphoreType.DMA((4,)),
    stat_c_sem=pltpu.SemaphoreType.DMA((1,)),
)


class Box:
    pass


def kernel(constraint, pattern, objective, row_bound, lower, upper, primal, dual, norms, *refs):
    b = Box()
    b.__dict__.update(zip(SCRATCH, refs))
    b.primal, b.dual = primal, dual
    y, c, z, x = (lax.axis_index(name) for name in ("y", "c", "z", "x"))
    other = 1 - c

    barrier = pltpu.get_barrier_semaphore()
    peers = 0
    for name, size, me in (("y", NY, y), ("c", NC, c), ("z", NZ, z), ("x", NX, x)):
        for step in range(1, size):
            pl.semaphore_signal(barrier, inc=1, device_id={name: (me + step) % size}, device_id_type=MESH)
            peers += 1

    def z_target(s):
        return (z + jnp.where(s % 2 == 1, 4 - (s + 1) // 2, 4 + s // 2)) % NZ

    def z_source(s):
        return (z + jnp.where(s % 2 == 1, (s + 1) // 2, NZ - s // 2)) % NZ

    load_objective = pltpu.make_async_copy(objective, b.objective, b.load_sem.at[8])
    load_objective.start()

    def load_matrix(s):
        group = aligned(z_target(s), GROUP)
        return pltpu.make_async_copy(constraint.at[group], b.matrix.at[group], b.load_sem.at[s])

    for s in range(NZ):
        load_matrix(s).start()
    load_bound = pltpu.make_async_copy(row_bound, b.bound, b.load_sem.at[9])
    load_bound.start()

    def spread(i, carry):
        at = aligned(i, BLOCK)
        b.lower[at] = jnp.broadcast_to(lower[pl.ds(i, 1)], (BLOCK, BLOCK)).T
        b.upper[at] = jnp.broadcast_to(upper[pl.ds(i, 1)], (BLOCK, BLOCK)).T
        return carry

    lax.fori_loop(0, 16, spread, 0)

    def wide(values):
        return jnp.concatenate([values, values], axis=1)

    def new_primal(at, gradient, it):
        low, high = wide(b.lower[at]), wide(b.upper[at])
        if it == 0:
            updated = jnp.clip(-step_primal * gradient, low, high)
            moved = updated
            b.extra[at] = (2.0 * updated).astype(BF16)
        else:
            before = b.primal[at]
            updated = jnp.clip(before - step_primal * gradient, low, high)
            moved = updated - before
            b.extra[at] = (2.0 * updated - before).astype(BF16)
        b.primal[at] = updated
        b.movement[it] += folded(moved * moved)

    b.movement[...] = jnp.zeros_like(b.movement)
    b.violation[...] = jnp.zeros_like(b.violation)

    load_objective.wait()

    def first(i, carry):
        at = aligned(i, GROUP)
        new_primal(at, b.objective[at], 0)
        return carry

    lax.fori_loop(0, 8, first, 0)

    def mask_group(group):
        for h in range(2):
            at = aligned(group * 2 + h, BLOCK)
            for j in range(16):
                keep = pattern[group * 2 + h, j].astype(F32).astype(BF16)
                cols = pl.ds(j * BLOCK, BLOCK)
                b.matrix[at, cols] = b.matrix[at, cols] * keep

    def turn_group(group):
        eye = jnp.where(
            lax.broadcasted_iota(jnp.int32, (256, 256), 0) == lax.broadcasted_iota(jnp.int32, (256, 256), 1), 1.0, 0.0
        ).astype(BF16)
        at = aligned(group, GROUP)
        for j in range(8):
            cols = pl.ds(j * 256, 256)
            b.turned[cols, at] = lax.dot_general(
                eye, b.matrix[at, cols], (((1,), (1,)), ((), ())), preferred_element_type=F32
            ).astype(BF16)

    def column_sum(it):
        ring = Ring(
            "x", NZ, b.x_from_prev.at[it], b.x_from_next.at[it], b.x_half_prev.at[it], b.x_half_next.at[it],
            (b.x_send_sem.at[it], b.x_half_prev_sem.at[it], b.x_half_next_sem.at[it], b.x_prev_sem.at[it],
             b.x_next_sem.at[it], b.x_gather_sem.at[it], b.x_gather_send.at[it]),
        )
        rows = b.rows.at[it]

        def piece(group, owner):
            return rows.at[group, owner]

        def z_copy(s):
            return pltpu.make_async_remote_copy(
                src_ref=b.z_send.at[s], dst_ref=b.z_recv.at[it, s], send_sem=b.z_send_sem.at[it],
                recv_sem=b.z_recv_sem.at[it, s], device_id={"z": z_target(s)}, device_id_type=MESH,
            )

        def summing(t, carry):
            @pl.when(t < NZ)
            def _():
                group = z_target(t)
                product = jnp.dot(b.matrix[aligned(group, GROUP)], b.extra[...], preferred_element_type=F32)
                b.part_x[t] = product.astype(BF16).reshape(NX, S, K)
                ring.begin(b.part_x, t)

            @pl.when((t >= LS) & (t < NZ + LS))
            def _():
                ring.relay(b.part_x, t - LS)

            @pl.when(t >= 2 * LS)
            def _():
                s = t - 2 * LS
                total = ring.total(b.part_x, s)

                @pl.when(s < NZ - 1)
                def _():
                    b.z_send[s] = total.astype(BF16)
                    z_copy(s).start()

                @pl.when(s == NZ - 1)
                def _():
                    b.share[...] = total

            return carry

        lax.fori_loop(0, NZ + 2 * LS, summing, 0)

        def adding(s, carry):
            arrived(b.z_recv.at[it, s], b.z_recv_sem.at[it, s])
            b.share[...] += b.z_recv[it, s].astype(F32)
            return carry

        lax.fori_loop(0, NZ - 1, adding, 0)
        rows[z, x] = b.share[...].astype(BF16)

        def z_spread(s, carry):
            to = z_source(s)
            mine = piece(z, x)
            pltpu.make_async_remote_copy(
                src_ref=mine, dst_ref=mine, send_sem=b.z_gather_send.at[it], recv_sem=b.z_gather_sem.at[it, z],
                device_id={"z": to}, device_id_type=MESH,
            ).start()
            return carry

        lax.fori_loop(1, NZ, z_spread, 0)

        if it == 0:
            load_bound.wait()
        if it == ITERS - 1:
            slack = b.bound[aligned(z * NX + x, S)] - b.share[...]
            over = jnp.maximum(slack, 0.0)
            b.violation[it] = folded(over * over)

        def gathering(t, carry):
            @pl.when(t < NZ)
            def _():
                group = z_source(t)

                @pl.when(t > 0)
                def _():
                    arrived(piece(group, x), b.z_gather_sem.at[it, group])

                ring.gather_begin(piece, group, t >= FAR_X)
                if it == 0:
                    turn_group(group)

            if it == ITERS - 1:
                stats(t)

            @pl.when((t >= LG) & (t < NZ + LG))
            def _():
                ring.gather_relay(piece, z_source(t - LG), t - LG >= FAR_X)

            @pl.when(t >= 2 * LG)
            def _():
                group = z_source(t - 2 * LG)
                ring.gather_end(piece, group)
                at = aligned(group, GROUP)
                slack = b.bound[at] - rows[group].reshape(GROUP, K).astype(F32)
                if it < ITERS - 1:
                    over = jnp.maximum(slack, 0.0)
                    b.violation[it] += folded(over * over)
                if it == 0:
                    dual = jnp.maximum(step_dual * slack, 0.0)
                else:
                    dual = jnp.maximum(b.dual[at] + step_dual * slack, 0.0)
                b.dual[at] = dual
                if it < ITERS - 1:
                    b.dual_bf[at] = dual.astype(BF16)

            return carry

        lax.fori_loop(0, NZ + 2 * LG, gathering, 0)
        ring.drain_sum(b.part_x)
        ring.drain_gather(b.part_x)
        arrived(b.z_send.at[pl.ds(0, NZ - 1)], b.z_send_sem.at[it])
        arrived(b.z_send.at[pl.ds(0, NZ - 1)], b.z_gather_send.at[it])

    def row_sum(it):
        n = it - 1
        ring = Ring(
            "y", NJ, b.y_from_prev.at[n], b.y_from_next.at[n], b.y_half_prev.at[n], b.y_half_next.at[n],
            (b.y_send_sem.at[n], b.y_half_prev_sem.at[n], b.y_half_next_sem.at[n], b.y_prev_sem.at[n],
             b.y_next_sem.at[n], b.y_gather_sem.at[n], b.y_gather_send.at[n]),
        )
        cols = b.cols.at[n]

        def piece(j, owner):
            return cols.at[j, c, owner]

        def swap(src, dst, send, recv):
            pltpu.make_async_remote_copy(
                src_ref=src, dst_ref=dst, send_sem=send, recv_sem=recv, device_id={"c": other}, device_id_type=MESH
            ).start()

        def product(j, core):
            return jnp.dot(b.turned[aligned(j * 2 + core, GROUP)], b.dual_bf[...], preferred_element_type=F32)

        def update(j, core):
            at = aligned(j * 2 + core, GROUP)
            new_primal(at, b.objective[at] - cols[j, core].reshape(GROUP, K).astype(F32), it)

        def body(t, carry):
            @pl.when(t < NJ)
            def _():
                b.core_send[t] = product(t, other).astype(BF16).reshape(NY, S, K)
                swap(b.core_send.at[t], b.core_recv.at[n, t], b.core_send_sem.at[n], b.core_recv_sem.at[n, t])

            @pl.when((t >= 1) & (t < NJ + 1))
            def _():
                j = t - 1
                own = product(j, c).reshape(NY, S, K)
                arrived(b.core_recv.at[n, j], b.core_recv_sem.at[n, j])
                b.part_y[j] = (own + b.core_recv[n, j].astype(F32)).astype(BF16)
                ring.begin(b.part_y, j)

            @pl.when((t >= 1 + LR) & (t < NJ + 1 + LR))
            def _():
                ring.relay(b.part_y, t - 1 - LR)

            @pl.when((t >= 1 + 2 * LR) & (t < NJ + 1 + 2 * LR))
            def _():
                j = t - 1 - 2 * LR
                cols[j, c, y] = ring.total(b.part_y, j).astype(BF16)
                ring.gather_begin(piece, j, j >= FAR_Y)

            @pl.when((t >= 1 + 3 * LR) & (t < NJ + 1 + 3 * LR))
            def _():
                ring.gather_relay(piece, t - 1 - 3 * LR, t - 1 - 3 * LR >= FAR_Y)

            @pl.when((t >= 1 + 4 * LR) & (t < NJ + 1 + 4 * LR))
            def _():
                j = t - 1 - 4 * LR
                ring.gather_end(piece, j)
                swap(cols.at[j, c], cols.at[j, c], b.core_gather_send.at[n], b.core_gather_sem.at[n, j])
                update(j, c)

            @pl.when(t >= 2 + 4 * LR)
            def _():
                j = t - 2 - 4 * LR
                arrived(cols.at[j, other], b.core_gather_sem.at[n, j])
                update(j, other)

            return carry

        lax.fori_loop(0, NJ + 2 + 4 * LR, body, 0)
        ring.drain_sum(b.part_y)
        ring.drain_gather(b.part_y)
        arrived(b.core_send, b.core_send_sem.at[n])
        arrived(b.core_send, b.core_gather_send.at[n])

    def stat_copy(src, dst, send, recv, to):
        pltpu.make_async_remote_copy(
            src_ref=src, dst_ref=dst, send_sem=b.stat_send_sem.at[send], recv_sem=recv, device_id=to, device_id_type=MESH
        ).start()

    def stacked(parts):
        sums = [jnp.sum(part, axis=0, keepdims=True) for part in parts]
        return jnp.concatenate(sums + [jnp.zeros((8 - len(parts), K), F32)], axis=0)

    def stats(t):
        @pl.when(t == 0)
        def _():
            b.stat_own[...] = stacked([b.violation[i] for i in range(3)])
            stat_copy(b.stat_own, b.stat_core, 0, b.stat_c_sem.at[0], {"c": other})

        @pl.when(t == 1)
        def _():
            arrived(b.stat_core, b.stat_c_sem.at[0])
            b.stat_pair[...] = b.stat_own[...] + b.stat_core[...]
            for step in range(1, NY):
                stat_copy(b.stat_pair, b.stat_y.at[step], 1, b.stat_y_sem.at[step], {"y": (y + step) % NY})

        @pl.when(t == NZ - 1)
        def _():
            total = b.stat_pair[...]
            for step in range(1, NY):
                arrived(b.stat_y.at[step], b.stat_y_sem.at[step])
                total += b.stat_y[step]
            b.kept[...] = total
            moved = stacked([b.movement[i] for i in range(3)])
            b.stat_row[...] = jnp.concatenate([moved[0:3], total[2:3], jnp.zeros((4, K), F32)], axis=0)
            for step in range(1, NZ):
                stat_copy(b.stat_row, b.stat_z.at[step], 2, b.stat_z_sem.at[step], {"z": (z + step) % NZ})

        @pl.when(t == NZ + 2 * LG - 2)
        def _():
            total = b.stat_row[...]
            for step in range(1, NZ):
                arrived(b.stat_z.at[step], b.stat_z_sem.at[step])
                total += b.stat_z[step]
            b.stat_col[...] = total
            for step in range(1, NX):
                stat_copy(b.stat_col, b.stat_x.at[step], 3, b.stat_x_sem.at[step], {"x": (x + step) % NX})

    def finish_stats():
        total = b.stat_col[...]
        for step in range(1, NX):
            arrived(b.stat_x.at[step], b.stat_x_sem.at[step])
            total += b.stat_x[step]
        over = jnp.concatenate([b.kept[0:2], total[3:4]], axis=0)
        each = jnp.sqrt(over / (2048 * NY * NC) + epsilon) + jnp.sqrt(total[0:3] / (2048 * NZ * NX) + epsilon)
        norms[...] = each[0:1] + each[1:2] + each[2:3]
        arrived(b.stat_core, b.stat_send_sem.at[0])
        arrived(b.stat_y.at[pl.ds(1, 3)], b.stat_send_sem.at[1])
        arrived(b.stat_z.at[pl.ds(1, 7)], b.stat_send_sem.at[2])
        arrived(b.stat_x.at[pl.ds(1, 3)], b.stat_send_sem.at[3])

    def prepare(t, carry):
        load_matrix(t).wait()
        mask_group(z_target(t))
        return carry

    lax.fori_loop(0, NZ, prepare, 0)
    pl.semaphore_wait(barrier, peers)
    column_sum(0)
    row_sum(1)
    column_sum(1)
    row_sum(2)

    column_sum(2)
    finish_stats()


def on_device(constraint, pattern, objective, row_bound, lower_bound, upper_bound):
    primal, dual, norms = pl.pallas_call(
        kernel,
        out_shape=(
            jax.ShapeDtypeStruct((2048, K), F32),
            jax.ShapeDtypeStruct((2048, K), F32),
            jax.ShapeDtypeStruct((1, K), F32),
        ),
        in_specs=[
            pl.BlockSpec(memory_space=pltpu.HBM),
            pl.BlockSpec(memory_space=pltpu.SMEM),
            pl.BlockSpec(memory_space=pltpu.HBM),
            pl.BlockSpec(memory_space=pltpu.HBM),
            pl.BlockSpec(memory_space=pltpu.VMEM),
            pl.BlockSpec(memory_space=pltpu.VMEM),
        ],
        out_specs=(
            pl.BlockSpec(memory_space=pltpu.VMEM),
            pl.BlockSpec(memory_space=pltpu.VMEM),
            pl.BlockSpec(memory_space=pltpu.VMEM),
        ),
        scratch_shapes=list(SCRATCH.values()),
        compiler_params=pltpu.CompilerParams(
            collective_id=0, has_side_effects=True, vmem_limit_bytes=48 * 1024 * 1024
        ),
        name="pdhg",
    )(constraint, pattern, objective, row_bound, lower_bound.reshape(16, BLOCK), upper_bound.reshape(16, BLOCK))
    return primal, dual, norms.reshape(K)


def solution(mesh):
    torus = Mesh(mesh.devices.reshape(NY, NC, NZ, NX), ("y", "c", "z", "x"))
    in_specs = (P(ROW, COL), P(ROW, COL), P(COL, None), P(ROW, None), P(COL), P(COL))
    out_specs = (P(COL, None), P(ROW, None), P())
    return jax.shard_map(on_device, mesh=torus, in_specs=in_specs, out_specs=out_specs, check_vma=False)
```

```python
import functools

import jax
import jax.numpy as jnp
from jax import lax
from jax.experimental import pallas as pl
from jax.experimental.pallas import tpu as pltpu
from jax.sharding import Mesh
from jax.sharding import PartitionSpec as P

MESH = pl.DeviceIdType.MESH
BF16 = jnp.bfloat16
F32 = jnp.float32
BLOCK = 128
ITERS = 3
NY, NC, NZ, NX = 4, 2, 8, 4
ROW = ("y", "c")
COL = ("z", "x")
K = 256
S = 64
HALF = S // 2
GROUP = NX * S
NJ = 4
LS = 4
LG = 4
LR = 3
FAR_X = 6
FAR_Y = 3
step_primal = 0.6
step_dual = 0.6
epsilon = 1e-6


def aligned(index, size):
    return pl.ds(pl.multiple_of(index * size, size), size)


def folded(values):
    return jnp.sum(values.reshape(-1, 8, values.shape[-1]), axis=0)


class Ring:
    def __init__(self, axis, groups, from_prev, from_next, half_prev, half_next, sems):
        self.axis, self.groups = axis, groups
        self.me = lax.axis_index(axis)
        self.next = (self.me + 1) % 4
        self.prev = (self.me + 3) % 4
        self.far = (self.me + 2) % 4
        self.from_prev, self.from_next = from_prev, from_next
        self.half_prev, self.half_next = half_prev, half_next
        self.send_sem, self.half_prev_sem, self.half_next_sem, self.prev_sem, self.next_sem, self.gather_sem, self.gather_send = sems

    def copy(self, src, dst, send, recv, to):
        pltpu.make_async_remote_copy(
            src_ref=src, dst_ref=dst, send_sem=send, recv_sem=recv, device_id={self.axis: to}, device_id_type=MESH
        ).start()

    def begin(self, part, s):
        low, high = pl.ds(0, HALF), pl.ds(HALF, HALF)
        self.copy(part.at[s, self.far, low], self.half_prev.at[s], self.send_sem, self.half_prev_sem.at[s], self.next)
        self.copy(part.at[s, self.far, high], self.half_next.at[s], self.send_sem, self.half_next_sem.at[s], self.prev)

    def relay(self, part, s):
        low, high = pl.ds(0, HALF), pl.ds(HALF, HALF)
        arrived(self.half_prev.at[s], self.half_prev_sem.at[s])
        part[s, self.next, low] = (part[s, self.next, low].astype(F32) + self.half_prev[s].astype(F32)).astype(BF16)
        self.copy(part.at[s, self.next], self.from_prev.at[s], self.send_sem, self.prev_sem.at[s], self.next)
        arrived(self.half_next.at[s], self.half_next_sem.at[s])
        part[s, self.prev, high] = (part[s, self.prev, high].astype(F32) + self.half_next[s].astype(F32)).astype(BF16)
        self.copy(part.at[s, self.prev], self.from_next.at[s], self.send_sem, self.next_sem.at[s], self.prev)

    def total(self, part, s):
        arrived(self.from_prev.at[s], self.prev_sem.at[s])
        arrived(self.from_next.at[s], self.next_sem.at[s])
        return part[s, self.me].astype(F32) + self.from_prev[s].astype(F32) + self.from_next[s].astype(F32)

    def gather_begin(self, piece, s, direct):
        low, high = pl.ds(0, HALF), pl.ds(HALF, HALF)
        mine = piece(s, self.me)
        self.copy(mine.at[low], mine.at[low], self.gather_send, self.gather_sem.at[0, s], self.next)
        self.copy(mine.at[high], mine.at[high], self.gather_send, self.gather_sem.at[1, s], self.prev)
        self.copy(mine.at[high], mine.at[high], self.gather_send, self.gather_sem.at[2, s], self.next)
        self.copy(mine.at[low], mine.at[low], self.gather_send, self.gather_sem.at[3, s], self.prev)

        @pl.when(direct)
        def _():
            self.copy(mine.at[low], mine.at[low], self.gather_send, self.gather_sem.at[4, s], self.far)
            self.copy(mine.at[high], mine.at[high], self.gather_send, self.gather_sem.at[5, s], self.far)

    def gather_relay(self, piece, s, direct):
        low, high = pl.ds(0, HALF), pl.ds(HALF, HALF)
        left, right = piece(s, self.prev), piece(s, self.next)
        arrived(left.at[low], self.gather_sem.at[0, s])

        @pl.when(jnp.logical_not(direct))
        def _():
            self.copy(left.at[low], left.at[low], self.gather_send, self.gather_sem.at[4, s], self.next)

        arrived(right.at[high], self.gather_sem.at[1, s])

        @pl.when(jnp.logical_not(direct))
        def _():
            self.copy(right.at[high], right.at[high], self.gather_send, self.gather_sem.at[5, s], self.prev)

    def gather_end(self, piece, s):
        low, high = pl.ds(0, HALF), pl.ds(HALF, HALF)
        left, right, far = piece(s, self.prev), piece(s, self.next), piece(s, self.far)
        arrived(left.at[high], self.gather_sem.at[2, s])
        arrived(right.at[low], self.gather_sem.at[3, s])
        arrived(far.at[low], self.gather_sem.at[4, s])
        arrived(far.at[high], self.gather_sem.at[5, s])

    def drain_sum(self, part):
        view = part.at[:, pl.ds(0, 3)]
        arrived(view, self.send_sem)

    def drain_gather(self, part):
        view = part.at[:, pl.ds(0, 3)]
        arrived(view, self.gather_send)


def arrived(ref, sem):
    pltpu.make_async_copy(ref, ref, sem).wait()


SCRATCH = dict(
    matrix=pltpu.VMEM((2048, 2048), BF16),
    turned=pltpu.VMEM((2048, 2048), BF16),
    objective=pltpu.VMEM((2048, K), F32),
    bound=pltpu.VMEM((2048, K), F32),
    extra=pltpu.VMEM((2048, K), BF16),
    dual_bf=pltpu.VMEM((2048, K), BF16),
    lower=pltpu.VMEM((2048, BLOCK), F32),
    upper=pltpu.VMEM((2048, BLOCK), F32),
    part_x=pltpu.VMEM((NZ, NX, S, K), BF16),
    x_from_prev=pltpu.VMEM((3, NZ, S, K), BF16),
    x_from_next=pltpu.VMEM((3, NZ, S, K), BF16),
    x_half_prev=pltpu.VMEM((3, NZ, HALF, K), BF16),
    x_half_next=pltpu.VMEM((3, NZ, HALF, K), BF16),
    z_send=pltpu.VMEM((NZ, S, K), BF16),
    z_recv=pltpu.VMEM((3, NZ, S, K), BF16),
    share=pltpu.VMEM((S, K), F32),
    rows=pltpu.VMEM((3, NZ, NX, S, K), BF16),
    core_send=pltpu.VMEM((NJ, NY, S, K), BF16),
    core_recv=pltpu.VMEM((2, NJ, NY, S, K), BF16),
    part_y=pltpu.VMEM((NJ, NY, S, K), BF16),
    y_from_prev=pltpu.VMEM((2, NJ, S, K), BF16),
    y_from_next=pltpu.VMEM((2, NJ, S, K), BF16),
    y_half_prev=pltpu.VMEM((2, NJ, HALF, K), BF16),
    y_half_next=pltpu.VMEM((2, NJ, HALF, K), BF16),
    cols=pltpu.VMEM((2, NJ, NC, NY, S, K), BF16),
    violation=pltpu.VMEM((3, 8, K), F32),
    movement=pltpu.VMEM((3, 8, K), F32),
    stat_own=pltpu.VMEM((8, K), F32),
    stat_pair=pltpu.VMEM((8, K), F32),
    stat_row=pltpu.VMEM((8, K), F32),
    stat_col=pltpu.VMEM((8, K), F32),
    stat_core=pltpu.VMEM((8, K), F32),
    stat_y=pltpu.VMEM((4, 8, K), F32),
    stat_z=pltpu.VMEM((8, 8, K), F32),
    stat_x=pltpu.VMEM((4, 8, K), F32),
    kept=pltpu.VMEM((8, K), F32),
    load_sem=pltpu.SemaphoreType.DMA((16,)),
    x_send_sem=pltpu.SemaphoreType.DMA((3,)),
    x_half_prev_sem=pltpu.SemaphoreType.DMA((3, NZ)),
    x_half_next_sem=pltpu.SemaphoreType.DMA((3, NZ)),
    x_prev_sem=pltpu.SemaphoreType.DMA((3, NZ)),
    x_next_sem=pltpu.SemaphoreType.DMA((3, NZ)),
    x_gather_sem=pltpu.SemaphoreType.DMA((3, 6, NZ)),
    x_gather_send=pltpu.SemaphoreType.DMA((3,)),
    z_send_sem=pltpu.SemaphoreType.DMA((3,)),
    z_recv_sem=pltpu.SemaphoreType.DMA((3, NZ)),
    z_gather_send=pltpu.SemaphoreType.DMA((3,)),
    z_gather_sem=pltpu.SemaphoreType.DMA((3, NZ)),
    core_send_sem=pltpu.SemaphoreType.DMA((2,)),
    core_recv_sem=pltpu.SemaphoreType.DMA((2, NJ)),
    core_gather_send=pltpu.SemaphoreType.DMA((2,)),
    core_gather_sem=pltpu.SemaphoreType.DMA((2, NJ)),
    y_send_sem=pltpu.SemaphoreType.DMA((2,)),
    y_half_prev_sem=pltpu.SemaphoreType.DMA((2, NJ)),
    y_half_next_sem=pltpu.SemaphoreType.DMA((2, NJ)),
    y_prev_sem=pltpu.SemaphoreType.DMA((2, NJ)),
    y_next_sem=pltpu.SemaphoreType.DMA((2, NJ)),
    y_gather_sem=pltpu.SemaphoreType.DMA((2, 6, NJ)),
    y_gather_send=pltpu.SemaphoreType.DMA((2,)),
    stat_send_sem=pltpu.SemaphoreType.DMA((4,)),
    stat_x_sem=pltpu.SemaphoreType.DMA((4,)),
    stat_z_sem=pltpu.SemaphoreType.DMA((8,)),
    stat_y_sem=pltpu.SemaphoreType.DMA((4,)),
    stat_c_sem=pltpu.SemaphoreType.DMA((1,)),
)


class Box:
    pass


def kernel(constraint, pattern, objective, row_bound, lower, upper, primal, dual, norms, *refs):
    b = Box()
    b.__dict__.update(zip(SCRATCH, refs))
    b.primal, b.dual = primal, dual
    y, c, z, x = (lax.axis_index(name) for name in ("y", "c", "z", "x"))
    other = 1 - c

    barrier = pltpu.get_barrier_semaphore()
    peers = 0
    for name, size, me in (("y", NY, y), ("c", NC, c), ("z", NZ, z), ("x", NX, x)):
        for step in range(1, size):
            pl.semaphore_signal(barrier, inc=1, device_id={name: (me + step) % size}, device_id_type=MESH)
            peers += 1

    def z_target(s):
        return (z + jnp.where(s % 2 == 1, 4 - (s + 1) // 2, 4 + s // 2)) % NZ

    def z_source(s):
        return (z + jnp.where(s % 2 == 1, (s + 1) // 2, NZ - s // 2)) % NZ

    load_objective = pltpu.make_async_copy(objective, b.objective, b.load_sem.at[8])
    load_objective.start()

    def load_matrix(s):
        group = aligned(z_target(s), GROUP)
        return pltpu.make_async_copy(constraint.at[group], b.matrix.at[group], b.load_sem.at[s])

    for s in range(NZ):
        load_matrix(s).start()
    load_bound = pltpu.make_async_copy(row_bound, b.bound, b.load_sem.at[9])
    load_bound.start()

    def spread(i, carry):
        at = aligned(i, BLOCK)
        b.lower[at] = jnp.broadcast_to(lower[pl.ds(i, 1)], (BLOCK, BLOCK)).T
        b.upper[at] = jnp.broadcast_to(upper[pl.ds(i, 1)], (BLOCK, BLOCK)).T
        return carry

    lax.fori_loop(0, 16, spread, 0)

    def wide(values):
        return jnp.concatenate([values, values], axis=1)

    def new_primal(at, gradient, it):
        low, high = wide(b.lower[at]), wide(b.upper[at])
        if it == 0:
            updated = jnp.clip(-step_primal * gradient, low, high)
            moved = updated
            b.extra[at] = (2.0 * updated).astype(BF16)
        else:
            before = b.primal[at]
            updated = jnp.clip(before - step_primal * gradient, low, high)
            moved = updated - before
            b.extra[at] = (2.0 * updated - before).astype(BF16)
        b.primal[at] = updated
        b.movement[it] += folded(moved * moved)

    b.movement[...] = jnp.zeros_like(b.movement)
    b.violation[...] = jnp.zeros_like(b.violation)

    load_objective.wait()

    def first(i, carry):
        at = aligned(i, GROUP)
        new_primal(at, b.objective[at], 0)
        return carry

    lax.fori_loop(0, 8, first, 0)

    def mask_group(group):
        for h in range(2):
            at = aligned(group * 2 + h, BLOCK)
            for j in range(16):
                keep = pattern[group * 2 + h, j].astype(F32).astype(BF16)
                cols = pl.ds(j * BLOCK, BLOCK)
                b.matrix[at, cols] = b.matrix[at, cols] * keep

    def turn_group(group):
        eye = jnp.where(
            lax.broadcasted_iota(jnp.int32, (256, 256), 0) == lax.broadcasted_iota(jnp.int32, (256, 256), 1), 1.0, 0.0
        ).astype(BF16)
        at = aligned(group, GROUP)
        for j in range(8):
            cols = pl.ds(j * 256, 256)
            b.turned[cols, at] = lax.dot_general(
                eye, b.matrix[at, cols], (((1,), (1,)), ((), ())), preferred_element_type=F32
            ).astype(BF16)

    def column_sum(it):
        ring = Ring(
            "x", NZ, b.x_from_prev.at[it], b.x_from_next.at[it], b.x_half_prev.at[it], b.x_half_next.at[it],
            (b.x_send_sem.at[it], b.x_half_prev_sem.at[it], b.x_half_next_sem.at[it], b.x_prev_sem.at[it],
             b.x_next_sem.at[it], b.x_gather_sem.at[it], b.x_gather_send.at[it]),
        )
        rows = b.rows.at[it]

        def piece(group, owner):
            return rows.at[group, owner]

        def z_copy(s):
            return pltpu.make_async_remote_copy(
                src_ref=b.z_send.at[s], dst_ref=b.z_recv.at[it, s], send_sem=b.z_send_sem.at[it],
                recv_sem=b.z_recv_sem.at[it, s], device_id={"z": z_target(s)}, device_id_type=MESH,
            )

        def summing(t, carry):
            @pl.when(t < NZ)
            def _():
                group = z_target(t)
                product = jnp.dot(b.matrix[aligned(group, GROUP)], b.extra[...], preferred_element_type=F32)
                b.part_x[t] = product.astype(BF16).reshape(NX, S, K)
                ring.begin(b.part_x, t)

            @pl.when((t >= LS) & (t < NZ + LS))
            def _():
                ring.relay(b.part_x, t - LS)

            @pl.when(t >= 2 * LS)
            def _():
                s = t - 2 * LS
                total = ring.total(b.part_x, s)

                @pl.when(s < NZ - 1)
                def _():
                    b.z_send[s] = total.astype(BF16)
                    z_copy(s).start()

                @pl.when(s == NZ - 1)
                def _():
                    b.share[...] = total

            return carry

        lax.fori_loop(0, NZ + 2 * LS, summing, 0)

        def adding(s, carry):
            arrived(b.z_recv.at[it, s], b.z_recv_sem.at[it, s])
            b.share[...] += b.z_recv[it, s].astype(F32)
            return carry

        lax.fori_loop(0, NZ - 1, adding, 0)
        rows[z, x] = b.share[...].astype(BF16)

        def z_spread(s, carry):
            to = z_source(s)
            mine = piece(z, x)
            pltpu.make_async_remote_copy(
                src_ref=mine, dst_ref=mine, send_sem=b.z_gather_send.at[it], recv_sem=b.z_gather_sem.at[it, z],
                device_id={"z": to}, device_id_type=MESH,
            ).start()
            return carry

        lax.fori_loop(1, NZ, z_spread, 0)

        if it == 0:
            load_bound.wait()
        if it == ITERS - 1:
            slack = b.bound[aligned(z * NX + x, S)] - b.share[...]
            over = jnp.maximum(slack, 0.0)
            b.violation[it] = folded(over * over)

        def gathering(t, carry):
            @pl.when(t < NZ)
            def _():
                group = z_source(t)

                @pl.when(t > 0)
                def _():
                    arrived(piece(group, x), b.z_gather_sem.at[it, group])

                ring.gather_begin(piece, group, t >= FAR_X)
                if it == 0:
                    turn_group(group)

            if it == ITERS - 1:
                stats(t)

            @pl.when((t >= LG) & (t < NZ + LG))
            def _():
                ring.gather_relay(piece, z_source(t - LG), t - LG >= FAR_X)

            @pl.when(t >= 2 * LG)
            def _():
                group = z_source(t - 2 * LG)
                ring.gather_end(piece, group)
                at = aligned(group, GROUP)
                slack = b.bound[at] - rows[group].reshape(GROUP, K).astype(F32)
                if it < ITERS - 1:
                    over = jnp.maximum(slack, 0.0)
                    b.violation[it] += folded(over * over)
                if it == 0:
                    dual = jnp.maximum(step_dual * slack, 0.0)
                else:
                    dual = jnp.maximum(b.dual[at] + step_dual * slack, 0.0)
                b.dual[at] = dual
                if it < ITERS - 1:
                    b.dual_bf[at] = dual.astype(BF16)

            return carry

        lax.fori_loop(0, NZ + 2 * LG, gathering, 0)
        ring.drain_sum(b.part_x)
        ring.drain_gather(b.part_x)
        arrived(b.z_send.at[pl.ds(0, NZ - 1)], b.z_send_sem.at[it])
        arrived(b.z_send.at[pl.ds(0, NZ - 1)], b.z_gather_send.at[it])

    def row_sum(it):
        n = it - 1
        ring = Ring(
            "y", NJ, b.y_from_prev.at[n], b.y_from_next.at[n], b.y_half_prev.at[n], b.y_half_next.at[n],
            (b.y_send_sem.at[n], b.y_half_prev_sem.at[n], b.y_half_next_sem.at[n], b.y_prev_sem.at[n],
             b.y_next_sem.at[n], b.y_gather_sem.at[n], b.y_gather_send.at[n]),
        )
        cols = b.cols.at[n]

        def piece(j, owner):
            return cols.at[j, c, owner]

        def swap(src, dst, send, recv):
            pltpu.make_async_remote_copy(
                src_ref=src, dst_ref=dst, send_sem=send, recv_sem=recv, device_id={"c": other}, device_id_type=MESH
            ).start()

        def product(j, core):
            return jnp.dot(b.turned[aligned(j * 2 + core, GROUP)], b.dual_bf[...], preferred_element_type=F32)

        def update(j, core):
            at = aligned(j * 2 + core, GROUP)
            new_primal(at, b.objective[at] - cols[j, core].reshape(GROUP, K).astype(F32), it)

        def body(t, carry):
            @pl.when(t < NJ)
            def _():
                b.core_send[t] = product(t, other).astype(BF16).reshape(NY, S, K)
                swap(b.core_send.at[t], b.core_recv.at[n, t], b.core_send_sem.at[n], b.core_recv_sem.at[n, t])

            @pl.when((t >= 1) & (t < NJ + 1))
            def _():
                j = t - 1
                own = product(j, c).reshape(NY, S, K)
                arrived(b.core_recv.at[n, j], b.core_recv_sem.at[n, j])
                b.part_y[j] = (own + b.core_recv[n, j].astype(F32)).astype(BF16)
                ring.begin(b.part_y, j)

            @pl.when((t >= 1 + LR) & (t < NJ + 1 + LR))
            def _():
                ring.relay(b.part_y, t - 1 - LR)

            @pl.when((t >= 1 + 2 * LR) & (t < NJ + 1 + 2 * LR))
            def _():
                j = t - 1 - 2 * LR
                cols[j, c, y] = ring.total(b.part_y, j).astype(BF16)
                ring.gather_begin(piece, j, j >= FAR_Y)

            @pl.when((t >= 1 + 3 * LR) & (t < NJ + 1 + 3 * LR))
            def _():
                ring.gather_relay(piece, t - 1 - 3 * LR, t - 1 - 3 * LR >= FAR_Y)

            @pl.when((t >= 1 + 4 * LR) & (t < NJ + 1 + 4 * LR))
            def _():
                j = t - 1 - 4 * LR
                ring.gather_end(piece, j)
                swap(cols.at[j, c], cols.at[j, c], b.core_gather_send.at[n], b.core_gather_sem.at[n, j])
                update(j, c)

            @pl.when(t >= 2 + 4 * LR)
            def _():
                j = t - 2 - 4 * LR
                arrived(cols.at[j, other], b.core_gather_sem.at[n, j])
                update(j, other)

            return carry

        lax.fori_loop(0, NJ + 2 + 4 * LR, body, 0)
        ring.drain_sum(b.part_y)
        ring.drain_gather(b.part_y)
        arrived(b.core_send, b.core_send_sem.at[n])
        arrived(b.core_send, b.core_gather_send.at[n])

    def stat_copy(src, dst, send, recv, to):
        pltpu.make_async_remote_copy(
            src_ref=src, dst_ref=dst, send_sem=b.stat_send_sem.at[send], recv_sem=recv, device_id=to, device_id_type=MESH
        ).start()

    def stacked(parts):
        sums = [jnp.sum(part, axis=0, keepdims=True) for part in parts]
        return jnp.concatenate(sums + [jnp.zeros((8 - len(parts), K), F32)], axis=0)

    def stats(t):
        @pl.when(t == 0)
        def _():
            b.stat_own[...] = stacked([b.violation[i] for i in range(3)])
            stat_copy(b.stat_own, b.stat_core, 0, b.stat_c_sem.at[0], {"c": other})

        @pl.when(t == 1)
        def _():
            arrived(b.stat_core, b.stat_c_sem.at[0])
            b.stat_pair[...] = b.stat_own[...] + b.stat_core[...]
            for step in range(1, NY):
                stat_copy(b.stat_pair, b.stat_y.at[step], 1, b.stat_y_sem.at[step], {"y": (y + step) % NY})

        @pl.when(t == NZ - 1)
        def _():
            total = b.stat_pair[...]
            for step in range(1, NY):
                arrived(b.stat_y.at[step], b.stat_y_sem.at[step])
                total += b.stat_y[step]
            b.kept[...] = total
            moved = stacked([b.movement[i] for i in range(3)])
            b.stat_row[...] = jnp.concatenate([moved[0:3], total[2:3], jnp.zeros((4, K), F32)], axis=0)
            for step in range(1, NZ):
                stat_copy(b.stat_row, b.stat_z.at[step], 2, b.stat_z_sem.at[step], {"z": (z + step) % NZ})

        @pl.when(t == NZ + 2 * LG - 2)
        def _():
            total = b.stat_row[...]
            for step in range(1, NZ):
                arrived(b.stat_z.at[step], b.stat_z_sem.at[step])
                total += b.stat_z[step]
            b.stat_col[...] = total
            for step in range(1, NX):
                stat_copy(b.stat_col, b.stat_x.at[step], 3, b.stat_x_sem.at[step], {"x": (x + step) % NX})

    def finish_stats():
        total = b.stat_col[...]
        for step in range(1, NX):
            arrived(b.stat_x.at[step], b.stat_x_sem.at[step])
            total += b.stat_x[step]
        over = jnp.concatenate([b.kept[0:2], total[3:4]], axis=0)
        each = jnp.sqrt(over / (2048 * NY * NC) + epsilon) + jnp.sqrt(total[0:3] / (2048 * NZ * NX) + epsilon)
        norms[...] = each[0:1] + each[1:2] + each[2:3]
        arrived(b.stat_core, b.stat_send_sem.at[0])
        arrived(b.stat_y.at[pl.ds(1, 3)], b.stat_send_sem.at[1])
        arrived(b.stat_z.at[pl.ds(1, 7)], b.stat_send_sem.at[2])
        arrived(b.stat_x.at[pl.ds(1, 3)], b.stat_send_sem.at[3])

    def prepare(t, carry):
        load_matrix(t).wait()
        mask_group(z_target(t))
        return carry

    lax.fori_loop(0, NZ, prepare, 0)
    pl.semaphore_wait(barrier, peers)
    column_sum(0)
    row_sum(1)
    column_sum(1)
    row_sum(2)

    column_sum(2)
    finish_stats()


def on_device(constraint, pattern, objective, row_bound, lower_bound, upper_bound):
    primal, dual, norms = pl.pallas_call(
        kernel,
        out_shape=(
            jax.ShapeDtypeStruct((2048, K), F32),
            jax.ShapeDtypeStruct((2048, K), F32),
            jax.ShapeDtypeStruct((1, K), F32),
        ),
        in_specs=[
            pl.BlockSpec(memory_space=pltpu.HBM),
            pl.BlockSpec(memory_space=pltpu.SMEM),
            pl.BlockSpec(memory_space=pltpu.HBM),
            pl.BlockSpec(memory_space=pltpu.HBM),
            pl.BlockSpec(memory_space=pltpu.VMEM),
            pl.BlockSpec(memory_space=pltpu.VMEM),
        ],
        out_specs=(
            pl.BlockSpec(memory_space=pltpu.VMEM),
            pl.BlockSpec(memory_space=pltpu.VMEM),
            pl.BlockSpec(memory_space=pltpu.VMEM),
        ),
        scratch_shapes=list(SCRATCH.values()),
        compiler_params=pltpu.CompilerParams(
            collective_id=0, has_side_effects=True, vmem_limit_bytes=48 * 1024 * 1024
        ),
        name="pdhg",
    )(constraint, pattern, objective, row_bound, lower_bound.reshape(16, BLOCK), upper_bound.reshape(16, BLOCK))
    return primal, dual, norms.reshape(K)


def solution(mesh):
    torus = Mesh(mesh.devices.reshape(NY, NC, NZ, NX), ("y", "c", "z", "x"))
    in_specs = (P(ROW, COL), P(ROW, COL), P(COL, None), P(ROW, None), P(COL), P(COL))
    out_specs = (P(COL, None), P(ROW, None), P())
    return jax.shard_map(on_device, mesh=torus, in_specs=in_specs, out_specs=out_specs, check_vma=False)
```

```python
import functools

import jax
import jax.numpy as jnp
from jax import lax
from jax.experimental import pallas as pl
from jax.experimental.pallas import tpu as pltpu
from jax.sharding import Mesh
from jax.sharding import PartitionSpec as P

MESH = pl.DeviceIdType.MESH
BF16 = jnp.bfloat16
F32 = jnp.float32
BLOCK = 128
ITERS = 3
NY, NC, NZ, NX = 4, 2, 8, 4
ROW = ("y", "c")
COL = ("z", "x")
K = 256
S = 64
HALF = S // 2
GROUP = NX * S
NJ = 4
LS = 4
LG = 4
LR = 3
FAR_X = 5
FAR_Y = 2
step_primal = 0.6
step_dual = 0.6
epsilon = 1e-6


def aligned(index, size):
    return pl.ds(pl.multiple_of(index * size, size), size)


def folded(values):
    return jnp.sum(values.reshape(-1, 8, values.shape[-1]), axis=0)


class Ring:
    def __init__(self, axis, groups, from_prev, from_next, half_prev, half_next, sems):
        self.axis, self.groups = axis, groups
        self.me = lax.axis_index(axis)
        self.next = (self.me + 1) % 4
        self.prev = (self.me + 3) % 4
        self.far = (self.me + 2) % 4
        self.from_prev, self.from_next = from_prev, from_next
        self.half_prev, self.half_next = half_prev, half_next
        self.send_sem, self.half_prev_sem, self.half_next_sem, self.prev_sem, self.next_sem, self.gather_sem, self.gather_send = sems

    def copy(self, src, dst, send, recv, to):
        pltpu.make_async_remote_copy(
            src_ref=src, dst_ref=dst, send_sem=send, recv_sem=recv, device_id={self.axis: to}, device_id_type=MESH
        ).start()

    def begin(self, part, s):
        low, high = pl.ds(0, HALF), pl.ds(HALF, HALF)
        self.copy(part.at[s, self.far, low], self.half_prev.at[s], self.send_sem, self.half_prev_sem.at[s], self.next)
        self.copy(part.at[s, self.far, high], self.half_next.at[s], self.send_sem, self.half_next_sem.at[s], self.prev)

    def relay(self, part, s):
        low, high = pl.ds(0, HALF), pl.ds(HALF, HALF)
        arrived(self.half_prev.at[s], self.half_prev_sem.at[s])
        part[s, self.next, low] = (part[s, self.next, low].astype(F32) + self.half_prev[s].astype(F32)).astype(BF16)
        self.copy(part.at[s, self.next], self.from_prev.at[s], self.send_sem, self.prev_sem.at[s], self.next)
        arrived(self.half_next.at[s], self.half_next_sem.at[s])
        part[s, self.prev, high] = (part[s, self.prev, high].astype(F32) + self.half_next[s].astype(F32)).astype(BF16)
        self.copy(part.at[s, self.prev], self.from_next.at[s], self.send_sem, self.next_sem.at[s], self.prev)

    def total(self, part, s):
        arrived(self.from_prev.at[s], self.prev_sem.at[s])
        arrived(self.from_next.at[s], self.next_sem.at[s])
        return part[s, self.me].astype(F32) + self.from_prev[s].astype(F32) + self.from_next[s].astype(F32)

    def gather_begin(self, piece, s, direct):
        low, high = pl.ds(0, HALF), pl.ds(HALF, HALF)
        mine = piece(s, self.me)
        self.copy(mine.at[low], mine.at[low], self.gather_send, self.gather_sem.at[0, s], self.next)
        self.copy(mine.at[high], mine.at[high], self.gather_send, self.gather_sem.at[1, s], self.prev)
        self.copy(mine.at[high], mine.at[high], self.gather_send, self.gather_sem.at[2, s], self.next)
        self.copy(mine.at[low], mine.at[low], self.gather_send, self.gather_sem.at[3, s], self.prev)

        @pl.when(direct)
        def _():
            self.copy(mine.at[low], mine.at[low], self.gather_send, self.gather_sem.at[4, s], self.far)
            self.copy(mine.at[high], mine.at[high], self.gather_send, self.gather_sem.at[5, s], self.far)

    def gather_relay(self, piece, s, direct):
        low, high = pl.ds(0, HALF), pl.ds(HALF, HALF)
        left, right = piece(s, self.prev), piece(s, self.next)
        arrived(left.at[low], self.gather_sem.at[0, s])

        @pl.when(jnp.logical_not(direct))
        def _():
            self.copy(left.at[low], left.at[low], self.gather_send, self.gather_sem.at[4, s], self.next)

        arrived(right.at[high], self.gather_sem.at[1, s])

        @pl.when(jnp.logical_not(direct))
        def _():
            self.copy(right.at[high], right.at[high], self.gather_send, self.gather_sem.at[5, s], self.prev)

    def gather_end(self, piece, s):
        low, high = pl.ds(0, HALF), pl.ds(HALF, HALF)
        left, right, far = piece(s, self.prev), piece(s, self.next), piece(s, self.far)
        arrived(left.at[high], self.gather_sem.at[2, s])
        arrived(right.at[low], self.gather_sem.at[3, s])
        arrived(far.at[low], self.gather_sem.at[4, s])
        arrived(far.at[high], self.gather_sem.at[5, s])

    def drain_sum(self, part):
        view = part.at[:, pl.ds(0, 3)]
        arrived(view, self.send_sem)

    def drain_gather(self, part):
        view = part.at[:, pl.ds(0, 3)]
        arrived(view, self.gather_send)


def arrived(ref, sem):
    pltpu.make_async_copy(ref, ref, sem).wait()


SCRATCH = dict(
    matrix=pltpu.VMEM((2048, 2048), BF16),
    turned=pltpu.VMEM((2048, 2048), BF16),
    objective=pltpu.VMEM((2048, K), F32),
    bound=pltpu.VMEM((2048, K), F32),
    extra=pltpu.VMEM((2048, K), BF16),
    dual_bf=pltpu.VMEM((2048, K), BF16),
    lower=pltpu.VMEM((2048, BLOCK), F32),
    upper=pltpu.VMEM((2048, BLOCK), F32),
    part_x=pltpu.VMEM((NZ, NX, S, K), BF16),
    x_from_prev=pltpu.VMEM((3, NZ, S, K), BF16),
    x_from_next=pltpu.VMEM((3, NZ, S, K), BF16),
    x_half_prev=pltpu.VMEM((3, NZ, HALF, K), BF16),
    x_half_next=pltpu.VMEM((3, NZ, HALF, K), BF16),
    z_send=pltpu.VMEM((NZ, S, K), BF16),
    z_recv=pltpu.VMEM((3, NZ, S, K), BF16),
    share=pltpu.VMEM((S, K), F32),
    rows=pltpu.VMEM((3, NZ, NX, S, K), BF16),
    core_send=pltpu.VMEM((NJ, NY, S, K), BF16),
    core_recv=pltpu.VMEM((2, NJ, NY, S, K), BF16),
    part_y=pltpu.VMEM((NJ, NY, S, K), BF16),
    y_from_prev=pltpu.VMEM((2, NJ, S, K), BF16),
    y_from_next=pltpu.VMEM((2, NJ, S, K), BF16),
    y_half_prev=pltpu.VMEM((2, NJ, HALF, K), BF16),
    y_half_next=pltpu.VMEM((2, NJ, HALF, K), BF16),
    cols=pltpu.VMEM((2, NJ, NC, NY, S, K), BF16),
    violation=pltpu.VMEM((3, 8, K), F32),
    movement=pltpu.VMEM((3, 8, K), F32),
    stat_own=pltpu.VMEM((8, K), F32),
    stat_pair=pltpu.VMEM((8, K), F32),
    stat_row=pltpu.VMEM((8, K), F32),
    stat_col=pltpu.VMEM((8, K), F32),
    stat_core=pltpu.VMEM((8, K), F32),
    stat_y=pltpu.VMEM((4, 8, K), F32),
    stat_z=pltpu.VMEM((8, 8, K), F32),
    stat_x=pltpu.VMEM((4, 8, K), F32),
    kept=pltpu.VMEM((8, K), F32),
    load_sem=pltpu.SemaphoreType.DMA((16,)),
    x_send_sem=pltpu.SemaphoreType.DMA((3,)),
    x_half_prev_sem=pltpu.SemaphoreType.DMA((3, NZ)),
    x_half_next_sem=pltpu.SemaphoreType.DMA((3, NZ)),
    x_prev_sem=pltpu.SemaphoreType.DMA((3, NZ)),
    x_next_sem=pltpu.SemaphoreType.DMA((3, NZ)),
    x_gather_sem=pltpu.SemaphoreType.DMA((3, 6, NZ)),
    x_gather_send=pltpu.SemaphoreType.DMA((3,)),
    z_send_sem=pltpu.SemaphoreType.DMA((3,)),
    z_recv_sem=pltpu.SemaphoreType.DMA((3, NZ)),
    z_gather_send=pltpu.SemaphoreType.DMA((3,)),
    z_gather_sem=pltpu.SemaphoreType.DMA((3, NZ)),
    core_send_sem=pltpu.SemaphoreType.DMA((2,)),
    core_recv_sem=pltpu.SemaphoreType.DMA((2, NJ)),
    core_gather_send=pltpu.SemaphoreType.DMA((2,)),
    core_gather_sem=pltpu.SemaphoreType.DMA((2, NJ)),
    y_send_sem=pltpu.SemaphoreType.DMA((2,)),
    y_half_prev_sem=pltpu.SemaphoreType.DMA((2, NJ)),
    y_half_next_sem=pltpu.SemaphoreType.DMA((2, NJ)),
    y_prev_sem=pltpu.SemaphoreType.DMA((2, NJ)),
    y_next_sem=pltpu.SemaphoreType.DMA((2, NJ)),
    y_gather_sem=pltpu.SemaphoreType.DMA((2, 6, NJ)),
    y_gather_send=pltpu.SemaphoreType.DMA((2,)),
    stat_send_sem=pltpu.SemaphoreType.DMA((4,)),
    stat_x_sem=pltpu.SemaphoreType.DMA((4,)),
    stat_z_sem=pltpu.SemaphoreType.DMA((8,)),
    stat_y_sem=pltpu.SemaphoreType.DMA((4,)),
    stat_c_sem=pltpu.SemaphoreType.DMA((1,)),
)


class Box:
    pass


def kernel(constraint, pattern, objective, row_bound, lower, upper, primal, dual, norms, *refs):
    b = Box()
    b.__dict__.update(zip(SCRATCH, refs))
    b.primal, b.dual = primal, dual
    y, c, z, x = (lax.axis_index(name) for name in ("y", "c", "z", "x"))
    other = 1 - c

    barrier = pltpu.get_barrier_semaphore()
    peers = 0
    for name, size, me in (("y", NY, y), ("c", NC, c), ("z", NZ, z), ("x", NX, x)):
        for step in range(1, size):
            pl.semaphore_signal(barrier, inc=1, device_id={name: (me + step) % size}, device_id_type=MESH)
            peers += 1

    def z_target(s):
        return (z + jnp.where(s % 2 == 1, 4 - (s + 1) // 2, 4 + s // 2)) % NZ

    def z_source(s):
        return (z + jnp.where(s % 2 == 1, (s + 1) // 2, NZ - s // 2)) % NZ

    load_objective = pltpu.make_async_copy(objective, b.objective, b.load_sem.at[8])
    load_objective.start()

    def load_matrix(s):
        group = aligned(z_target(s), GROUP)
        return pltpu.make_async_copy(constraint.at[group], b.matrix.at[group], b.load_sem.at[s])

    for s in range(NZ):
        load_matrix(s).start()
    load_bound = pltpu.make_async_copy(row_bound, b.bound, b.load_sem.at[9])
    load_bound.start()

    def spread(i, carry):
        at = aligned(i, BLOCK)
        b.lower[at] = jnp.broadcast_to(lower[pl.ds(i, 1)], (BLOCK, BLOCK)).T
        b.upper[at] = jnp.broadcast_to(upper[pl.ds(i, 1)], (BLOCK, BLOCK)).T
        return carry

    lax.fori_loop(0, 16, spread, 0)

    def wide(values):
        return jnp.concatenate([values, values], axis=1)

    def new_primal(at, gradient, it):
        low, high = wide(b.lower[at]), wide(b.upper[at])
        if it == 0:
            updated = jnp.clip(-step_primal * gradient, low, high)
            moved = updated
            b.extra[at] = (2.0 * updated).astype(BF16)
        else:
            before = b.primal[at]
            updated = jnp.clip(before - step_primal * gradient, low, high)
            moved = updated - before
            b.extra[at] = (2.0 * updated - before).astype(BF16)
        b.primal[at] = updated
        b.movement[it] += folded(moved * moved)

    b.movement[...] = jnp.zeros_like(b.movement)
    b.violation[...] = jnp.zeros_like(b.violation)

    load_objective.wait()

    def first(i, carry):
        at = aligned(i, GROUP)
        new_primal(at, b.objective[at], 0)
        return carry

    lax.fori_loop(0, 8, first, 0)

    def mask_group(group):
        for h in range(2):
            at = aligned(group * 2 + h, BLOCK)
            for j in range(16):
                keep = pattern[group * 2 + h, j].astype(F32).astype(BF16)
                cols = pl.ds(j * BLOCK, BLOCK)
                b.matrix[at, cols] = b.matrix[at, cols] * keep

    def turn_group(group):
        eye = jnp.where(
            lax.broadcasted_iota(jnp.int32, (256, 256), 0) == lax.broadcasted_iota(jnp.int32, (256, 256), 1), 1.0, 0.0
        ).astype(BF16)
        at = aligned(group, GROUP)
        for j in range(8):
            cols = pl.ds(j * 256, 256)
            b.turned[cols, at] = lax.dot_general(
                eye, b.matrix[at, cols], (((1,), (1,)), ((), ())), preferred_element_type=F32
            ).astype(BF16)

    def part_product(t):
        product = jnp.dot(b.matrix[aligned(z_target(t), GROUP)], b.extra[...], preferred_element_type=F32)
        b.part_x[t] = product.astype(BF16).reshape(NX, S, K)

    def column_sum(it):
        ring = Ring(
            "x", NZ, b.x_from_prev.at[it], b.x_from_next.at[it], b.x_half_prev.at[it], b.x_half_next.at[it],
            (b.x_send_sem.at[it], b.x_half_prev_sem.at[it], b.x_half_next_sem.at[it], b.x_prev_sem.at[it],
             b.x_next_sem.at[it], b.x_gather_sem.at[it], b.x_gather_send.at[it]),
        )
        rows = b.rows.at[it]

        def piece(group, owner):
            return rows.at[group, owner]

        def z_copy(s):
            return pltpu.make_async_remote_copy(
                src_ref=b.z_send.at[s], dst_ref=b.z_recv.at[it, s], send_sem=b.z_send_sem.at[it],
                recv_sem=b.z_recv_sem.at[it, s], device_id={"z": z_target(s)}, device_id_type=MESH,
            )

        def summing(t, carry):
            @pl.when(t < NZ)
            def _():

                @pl.when(t > (0 if it == 0 else -1))
                def _():
                    part_product(t)

                ring.begin(b.part_x, t)

            @pl.when((t >= LS) & (t < NZ + LS))
            def _():
                ring.relay(b.part_x, t - LS)

            @pl.when(t >= 2 * LS)
            def _():
                s = t - 2 * LS
                total = ring.total(b.part_x, s)

                @pl.when(s < NZ - 1)
                def _():
                    b.z_send[s] = total.astype(BF16)
                    z_copy(s).start()

                @pl.when(s == NZ - 1)
                def _():
                    b.share[...] = total

            return carry

        lax.fori_loop(0, NZ + 2 * LS, summing, 0)

        def adding(s, carry):
            arrived(b.z_recv.at[it, s], b.z_recv_sem.at[it, s])
            b.share[...] += b.z_recv[it, s].astype(F32)
            return carry

        lax.fori_loop(0, NZ - 1, adding, 0)
        rows[z, x] = b.share[...].astype(BF16)

        def z_spread(s, carry):
            to = z_source(s)
            mine = piece(z, x)
            pltpu.make_async_remote_copy(
                src_ref=mine, dst_ref=mine, send_sem=b.z_gather_send.at[it], recv_sem=b.z_gather_sem.at[it, z],
                device_id={"z": to}, device_id_type=MESH,
            ).start()
            return carry

        lax.fori_loop(1, NZ, z_spread, 0)

        if it == 0:
            load_bound.wait()
        if it == ITERS - 1:
            slack = b.bound[aligned(z * NX + x, S)] - b.share[...]
            over = jnp.maximum(slack, 0.0)
            b.violation[it] = folded(over * over)

        def gathering(t, carry):
            @pl.when(t < NZ)
            def _():
                group = z_source(t)

                @pl.when(t > 0)
                def _():
                    arrived(piece(group, x), b.z_gather_sem.at[it, group])

                ring.gather_begin(piece, group, t >= FAR_X)
                if it == 0:
                    turn_group(group)

            if it == ITERS - 1:
                stats(t)

            @pl.when((t >= LG) & (t < NZ + LG))
            def _():
                ring.gather_relay(piece, z_source(t - LG), t - LG >= FAR_X)

            @pl.when(t >= 2 * LG)
            def _():
                group = z_source(t - 2 * LG)
                ring.gather_end(piece, group)
                at = aligned(group, GROUP)
                slack = b.bound[at] - rows[group].reshape(GROUP, K).astype(F32)
                if it < ITERS - 1:
                    over = jnp.maximum(slack, 0.0)
                    b.violation[it] += folded(over * over)
                if it == 0:
                    dual = jnp.maximum(step_dual * slack, 0.0)
                else:
                    dual = jnp.maximum(b.dual[at] + step_dual * slack, 0.0)
                b.dual[at] = dual
                if it < ITERS - 1:
                    b.dual_bf[at] = dual.astype(BF16)

            return carry

        lax.fori_loop(0, NZ + 2 * LG, gathering, 0)
        ring.drain_sum(b.part_x)
        ring.drain_gather(b.part_x)
        arrived(b.z_send.at[pl.ds(0, NZ - 1)], b.z_send_sem.at[it])
        arrived(b.z_send.at[pl.ds(0, NZ - 1)], b.z_gather_send.at[it])

    def row_sum(it):
        n = it - 1
        ring = Ring(
            "y", NJ, b.y_from_prev.at[n], b.y_from_next.at[n], b.y_half_prev.at[n], b.y_half_next.at[n],
            (b.y_send_sem.at[n], b.y_half_prev_sem.at[n], b.y_half_next_sem.at[n], b.y_prev_sem.at[n],
             b.y_next_sem.at[n], b.y_gather_sem.at[n], b.y_gather_send.at[n]),
        )
        cols = b.cols.at[n]

        def piece(j, owner):
            return cols.at[j, c, owner]

        def swap(src, dst, send, recv):
            pltpu.make_async_remote_copy(
                src_ref=src, dst_ref=dst, send_sem=send, recv_sem=recv, device_id={"c": other}, device_id_type=MESH
            ).start()

        def product(j, core):
            return jnp.dot(b.turned[aligned(j * 2 + core, GROUP)], b.dual_bf[...], preferred_element_type=F32)

        def update(j, core):
            at = aligned(j * 2 + core, GROUP)
            new_primal(at, b.objective[at] - cols[j, core].reshape(GROUP, K).astype(F32), it)

        def body(t, carry):
            @pl.when(t < NJ)
            def _():
                b.core_send[t] = product(t, other).astype(BF16).reshape(NY, S, K)
                swap(b.core_send.at[t], b.core_recv.at[n, t], b.core_send_sem.at[n], b.core_recv_sem.at[n, t])

            @pl.when((t >= 1) & (t < NJ + 1))
            def _():
                j = t - 1
                own = product(j, c).reshape(NY, S, K)
                arrived(b.core_recv.at[n, j], b.core_recv_sem.at[n, j])
                b.part_y[j] = (own + b.core_recv[n, j].astype(F32)).astype(BF16)
                ring.begin(b.part_y, j)

            @pl.when((t >= 1 + LR) & (t < NJ + 1 + LR))
            def _():
                ring.relay(b.part_y, t - 1 - LR)

            @pl.when((t >= 1 + 2 * LR) & (t < NJ + 1 + 2 * LR))
            def _():
                j = t - 1 - 2 * LR
                cols[j, c, y] = ring.total(b.part_y, j).astype(BF16)
                ring.gather_begin(piece, j, j >= FAR_Y)

            @pl.when((t >= 1 + 3 * LR) & (t < NJ + 1 + 3 * LR))
            def _():
                ring.gather_relay(piece, t - 1 - 3 * LR, t - 1 - 3 * LR >= FAR_Y)

            @pl.when((t >= 1 + 4 * LR) & (t < NJ + 1 + 4 * LR))
            def _():
                j = t - 1 - 4 * LR
                ring.gather_end(piece, j)
                swap(cols.at[j, c], cols.at[j, c], b.core_gather_send.at[n], b.core_gather_sem.at[n, j])
                update(j, c)

            @pl.when(t >= 2 + 4 * LR)
            def _():
                j = t - 2 - 4 * LR
                arrived(cols.at[j, other], b.core_gather_sem.at[n, j])
                update(j, other)

            return carry

        lax.fori_loop(0, NJ + 2 + 4 * LR, body, 0)
        ring.drain_sum(b.part_y)
        ring.drain_gather(b.part_y)
        arrived(b.core_send, b.core_send_sem.at[n])
        arrived(b.core_send, b.core_gather_send.at[n])

    def stat_copy(src, dst, send, recv, to):
        pltpu.make_async_remote_copy(
            src_ref=src, dst_ref=dst, send_sem=b.stat_send_sem.at[send], recv_sem=recv, device_id=to, device_id_type=MESH
        ).start()

    def stacked(parts):
        sums = [jnp.sum(part, axis=0, keepdims=True) for part in parts]
        return jnp.concatenate(sums + [jnp.zeros((8 - len(parts), K), F32)], axis=0)

    def stats(t):
        @pl.when(t == 0)
        def _():
            b.stat_own[...] = stacked([b.violation[i] for i in range(3)])
            stat_copy(b.stat_own, b.stat_core, 0, b.stat_c_sem.at[0], {"c": other})

        @pl.when(t == 1)
        def _():
            arrived(b.stat_core, b.stat_c_sem.at[0])
            b.stat_pair[...] = b.stat_own[...] + b.stat_core[...]
            for step in range(1, NY):
                stat_copy(b.stat_pair, b.stat_y.at[step], 1, b.stat_y_sem.at[step], {"y": (y + step) % NY})

        @pl.when(t == NZ - 1)
        def _():
            total = b.stat_pair[...]
            for step in range(1, NY):
                arrived(b.stat_y.at[step], b.stat_y_sem.at[step])
                total += b.stat_y[step]
            b.kept[...] = total
            moved = stacked([b.movement[i] for i in range(3)])
            b.stat_row[...] = jnp.concatenate([moved[0:3], total[2:3], jnp.zeros((4, K), F32)], axis=0)
            for step in range(1, NZ):
                stat_copy(b.stat_row, b.stat_z.at[step], 2, b.stat_z_sem.at[step], {"z": (z + step) % NZ})

        @pl.when(t == NZ + 2 * LG - 2)
        def _():
            total = b.stat_row[...]
            for step in range(1, NZ):
                arrived(b.stat_z.at[step], b.stat_z_sem.at[step])
                total += b.stat_z[step]
            b.stat_col[...] = total
            for step in range(1, NX):
                stat_copy(b.stat_col, b.stat_x.at[step], 3, b.stat_x_sem.at[step], {"x": (x + step) % NX})

    def finish_stats():
        total = b.stat_col[...]
        for step in range(1, NX):
            arrived(b.stat_x.at[step], b.stat_x_sem.at[step])
            total += b.stat_x[step]
        over = jnp.concatenate([b.kept[0:2], total[3:4]], axis=0)
        each = jnp.sqrt(over / (2048 * NY * NC) + epsilon) + jnp.sqrt(total[0:3] / (2048 * NZ * NX) + epsilon)
        norms[...] = each[0:1] + each[1:2] + each[2:3]
        arrived(b.stat_core, b.stat_send_sem.at[0])
        arrived(b.stat_y.at[pl.ds(1, 3)], b.stat_send_sem.at[1])
        arrived(b.stat_z.at[pl.ds(1, 7)], b.stat_send_sem.at[2])
        arrived(b.stat_x.at[pl.ds(1, 3)], b.stat_send_sem.at[3])

    def prepare(t, carry):
        load_matrix(t).wait()
        mask_group(z_target(t))
        return carry

    lax.fori_loop(0, NZ, prepare, 0)
    part_product(0)
    pl.semaphore_wait(barrier, peers)
    column_sum(0)
    row_sum(1)
    column_sum(1)
    row_sum(2)

    column_sum(2)
    finish_stats()


def on_device(constraint, pattern, objective, row_bound, lower_bound, upper_bound):
    primal, dual, norms = pl.pallas_call(
        kernel,
        out_shape=(
            jax.ShapeDtypeStruct((2048, K), F32),
            jax.ShapeDtypeStruct((2048, K), F32),
            jax.ShapeDtypeStruct((1, K), F32),
        ),
        in_specs=[
            pl.BlockSpec(memory_space=pltpu.HBM),
            pl.BlockSpec(memory_space=pltpu.SMEM),
            pl.BlockSpec(memory_space=pltpu.HBM),
            pl.BlockSpec(memory_space=pltpu.HBM),
            pl.BlockSpec(memory_space=pltpu.VMEM),
            pl.BlockSpec(memory_space=pltpu.VMEM),
        ],
        out_specs=(
            pl.BlockSpec(memory_space=pltpu.VMEM),
            pl.BlockSpec(memory_space=pltpu.VMEM),
            pl.BlockSpec(memory_space=pltpu.VMEM),
        ),
        scratch_shapes=list(SCRATCH.values()),
        compiler_params=pltpu.CompilerParams(
            collective_id=0, has_side_effects=True, vmem_limit_bytes=48 * 1024 * 1024
        ),
        name="pdhg",
    )(constraint, pattern, objective, row_bound, lower_bound.reshape(16, BLOCK), upper_bound.reshape(16, BLOCK))
    return primal, dual, norms.reshape(K)


def solution(mesh):
    torus = Mesh(mesh.devices.reshape(NY, NC, NZ, NX), ("y", "c", "z", "x"))
    in_specs = (P(ROW, COL), P(ROW, COL), P(COL, None), P(ROW, None), P(COL), P(COL))
    out_specs = (P(COL, None), P(ROW, None), P())
    return jax.shard_map(on_device, mesh=torus, in_specs=in_specs, out_specs=out_specs, check_vma=False)
```
